32 devices in a mesh: dp: 8 (over y, x, core), tp: 4 (over z).
Axes of the slice: x: 2, y: 2, z: 4, core: 2. Of those that a mesh axis runs over, the one named last changes fastest.
Arguments:
- patches: bfloat16 [16384, 768], P(('dp', 'tp')), may hold values from -6 to 6
- validity: int32 [16, 1024], P('dp'), may hold values from 0 to 1, as said below
- mask_pos: int32 [16, 1024], P('dp'), may hold values 0 or 1
- mask_token: float32 [768], replicated, may hold values from -5 to 5
- ln1_gain: float32 [768], replicated, may hold values from 0.5 to 1.5
- ln1_bias: float32 [768], replicated, may hold values from -3 to 3
- w_qkv: bfloat16 [768, 3, 768], P(None, None, 'tp'), may hold values from -0.21875 to 0.21875
- b_qv: float32 [2, 768], P(None, 'tp'), may hold values from -3 to 3
- w_out: bfloat16 [768, 768], P('tp'), may hold values from -0.625 to 0.625
- b_out: float32 [768], replicated, may hold values from -3 to 3
- ln2_gain: float32 [768], replicated, may hold values from 0.5 to 1.5
- ln2_bias: float32 [768], replicated, may hold values from -3 to 3
- w_up: bfloat16 [768, 3072], P(None, 'tp'), may hold values from -0.21875 to 0.21875
- b_up: float32 [3072], P('tp'), may hold values from -3 to 3
- w_down: bfloat16 [3072, 768], P('tp'), may hold values from -0.109375 to 0.109375
- b_down: float32 [768], replicated, may hold values from -3 to 3
- out_grad: bfloat16 [16384, 768], P(('dp', 'tp')), may hold values from -6 to 6
Outputs:
- output: bfloat16 [16384, 768], P(('dp', 'tp'))
- grad_patches: float32 [16384, 768], P(('dp', 'tp'))
- grad_mask_token: float32 [768], replicated
- grad_ln1_gain: float32 [768], replicated
- grad_ln1_bias: float32 [768], replicated
- grad_w_qkv: float32 [768, 3, 768], P(None, None, 'tp')
- grad_b_qv: float32 [2, 768], P(None, 'tp')
- grad_w_out: float32 [768, 768], P('tp')
- grad_b_out: float32 [768], replicated
- grad_ln2_gain: float32 [768], replicated
- grad_ln2_bias: float32 [768], replicated
- grad_w_up: float32 [768, 3072], P(None, 'tp')
- grad_b_up: float32 [3072], P('tp')
- grad_w_down: float32 [3072, 768], P('tp')
- grad_b_down: float32 [768], replicated
The draws below stay inside these ranges and needn't reach their ends.
Inputs may be any that keep to these rules, and one draw needn't show every extreme that they name: `validity`: each bucket's valid slots are its first ones, at least 256 of them; buckets whose index is a multiple of 3 are full.
All inputs are finite; a program needn't handle non-finite values. No bound on the sum of `mask_pos` on one device may be relied on, other than what follows from the above.
Results may differ from the reference program's by a relative error of at most 0.017.
Values may be sent and summed in bfloat16 or wider, within the bound.
A program may use at most 128 MiB of HBM per device.

```python
from functools import partial
import jax
import jax.numpy as jnp
from jax import lax

D = 768
HEADS = 12
HEAD_DIM = 64
FF = 3072
SEQ = 1024
BUCKETS = 16
TOKENS = 16384
N_TP = 4


def draw_validity(key, part):
    lengths = jax.random.randint(key, (BUCKETS,), SEQ // 4, SEQ + 1)
    full_rows = jnp.arange(BUCKETS) % 3 == 0
    lengths = jnp.where(full_rows, SEQ, lengths)
    return (jnp.arange(SEQ)[None, :] < lengths[:, None]).astype(jnp.int32)


def place_ends(drawn, own_key, least, largest):
    index_at = [jax.random.randint(jax.random.fold_in(own_key, axis), (), 0, length) for axis, length in enumerate(drawn.shape)]
    longest = drawn.shape.index(max(drawn.shape))
    neighbour = index_at[:longest] + [(index_at[longest] + 1) % drawn.shape[longest]] + index_at[longest + 1:]
    return drawn.at[tuple(index_at)].set(least).at[tuple(neighbour)].set(largest)


def steps_of(rng, shape, split, least, top_value):
    def one(position, blocks):
        draws = jax.random.uniform(jax.random.fold_in(jax.random.fold_in(rng, 6), position), (blocks,), jnp.float32, least / len(split), top_value / len(split))
        return jnp.repeat(jnp.exp(draws), shape[position] // blocks).reshape((-1,) + (1,) * (len(shape) - position - 1))

    level = one(*split[0])
    for cut in split[1:]:
        level = level * one(*cut)
    return level


def scatter_about(rng, extent, scale, bound, split=(), kind=jnp.bfloat16):
    level = steps_of(rng, extent, split, -0.22, 0.18) if split else 1.0
    result = jax.random.normal(rng, extent, jnp.float32) * scale * level
    return jnp.minimum(jnp.maximum(result, -bound), bound).astype(kind)


def setup_inputs(seed: int = 0) -> dict:
    seeds = jax.random.split(jax.random.key(seed), 18)
    return {
        "patches": scatter_about(seeds[0], (TOKENS, D), 1.0, 6.0, ((0, 32),)),
        "validity": draw_validity(jax.random.fold_in(seeds[17], 71), 0),
        "mask_pos": place_ends((jax.random.randint(seeds[2], (BUCKETS, SEQ), 0, 5) < 2).astype(jnp.int32), jax.random.fold_in(seeds[2], 1), 0, 1),
        "mask_token": scatter_about(seeds[3], (D,), 1.0, 5.0, (), jnp.float32),
        "ln1_gain": jnp.clip(1.0 + 0.1 * jax.random.normal(seeds[4], (D,), jnp.float32), 0.5, 1.5),
        "ln1_bias": scatter_about(seeds[5], (D,), 0.5, 3.0, (), jnp.float32),
        "w_qkv": scatter_about(seeds[6], (D, 3, D), D ** -0.5, 0.21875, ((2, 4),)),
        "b_qv": scatter_about(seeds[7], (2, D), 0.5, 3.0, ((1, 4),), jnp.float32),
        "w_out": scatter_about(seeds[8], (D, D), (D // 8) ** -0.5, 0.625, ((0, 4),)),
        "b_out": scatter_about(seeds[9], (D,), 0.5, 3.0, (), jnp.float32),
        "ln2_gain": jnp.clip(1.0 + 0.1 * jax.random.normal(seeds[10], (D,), jnp.float32), 0.5, 1.5),
        "ln2_bias": scatter_about(seeds[11], (D,), 0.5, 3.0, (), jnp.float32),
        "w_up": scatter_about(seeds[12], (D, FF), D ** -0.5, 0.21875, ((1, 4),)),
        "b_up": scatter_about(seeds[13], (FF,), 0.5, 3.0, ((0, 4),), jnp.float32),
        "w_down": scatter_about(seeds[14], (FF, D), FF ** -0.5, 0.109375, ((0, 4),)),
        "b_down": scatter_about(seeds[15], (D,), 0.5, 3.0, (), jnp.float32),
        "out_grad": scatter_about(seeds[16], (TOKENS, D), 1.0, 6.0, ((0, 32),)),
    }


@jax.custom_vjp
def low(v):
    return lax.optimization_barrier(v.astype(jnp.bfloat16)).astype(jnp.float32)

@jax.custom_vjp
def low_back(v):
    return v

def low_keep(v):
    return (low(v), None)

def low_pass(kept, grad):
    return (grad,)

def back_keep(v):
    return (v, None)

def back_low(kept, grad):
    return (low(grad),)
low.defvjp(low_keep, low_pass)
low_back.defvjp(back_keep, back_low)

def layer_norm(values, gain, bias):
    center = values - lax.optimization_barrier(jnp.mean(values, -1, keepdims=True))
    spread = lax.optimization_barrier(jnp.mean(center * center, -1, keepdims=True))
    return center * lax.rsqrt(spread + 1e-06) * gain + bias

def attend(bucket_in):
    query_rows, key_rows, value_rows, keep_key = bucket_in
    highest = lax.Precision.HIGHEST
    scores = jnp.einsum('qhd,khd->hqk', query_rows, key_rows, precision=highest) * HEAD_DIM ** (-0.5)
    scores = low_back(jnp.where(keep_key[None, None, :] > 0, scores, -1000000000.0))
    weights = low(jax.nn.softmax(scores, axis=-1))
    return low(low_back(jnp.einsum('hqk,khd->qhd', weights, value_rows, precision=highest)))

def block_sum(left, right, count):
    highest = lax.Precision.HIGHEST
    width = left.shape[1] // count
    total = jnp.zeros((left.shape[0], right.shape[1]), jnp.float32)
    for index in range(count):
        term = jnp.dot(left[:, index * width:(index + 1) * width], right[index * width:(index + 1) * width], precision=highest)
        total = total + low(low_back(term))
    return total

def forward(valid_col, masked_col, validity, patches, mask_token, ln1_gain, ln1_bias, w_qkv, b_qv, w_out, b_out, ln2_gain, ln2_bias, w_up, b_up, w_down, b_down):
    highest = lax.Precision.HIGHEST
    block_in = valid_col * (1.0 - masked_col) * patches + valid_col * masked_col * mask_token[None, :]
    normed_one = low(layer_norm(block_in, ln1_gain, ln1_bias))

    def project(index, bias):
        return low(low_back(jnp.dot(normed_one, w_qkv[:, index, :], precision=highest) + bias))
    shape = (BUCKETS, SEQ, HEADS, HEAD_DIM)
    query_rows = project(0, b_qv[0]).reshape(shape)
    key_rows = project(1, jnp.zeros_like(b_qv[0])).reshape(shape)
    value_rows = project(2, b_qv[1]).reshape(shape)
    context = lax.map(jax.checkpoint(attend), (query_rows, key_rows, value_rows, validity))
    context = context.reshape(TOKENS, D)
    residual = block_in + block_sum(context, w_out, N_TP) + b_out
    normed_two = low(layer_norm(residual, ln2_gain, ln2_bias))
    hidden_pre = low_back(jnp.dot(normed_two, w_up, precision=highest) + b_up)
    hidden = low(jax.nn.gelu(hidden_pre, approximate=False))
    mlp_out = block_sum(hidden, w_down, N_TP) + b_down
    return valid_col * (residual + mlp_out)

def reference(patches, validity, mask_pos, mask_token, ln1_gain, ln1_bias, w_qkv, b_qv, w_out, b_out, ln2_gain, ln2_bias, w_up, b_up, w_down, b_down, out_grad):
    valid_col = validity.reshape(TOKENS, 1).astype(jnp.float32)
    masked_col = mask_pos.reshape(TOKENS, 1).astype(jnp.float32)
    params = (patches.astype(jnp.float32), mask_token, ln1_gain, ln1_bias, w_qkv.astype(jnp.float32), b_qv, w_out.astype(jnp.float32), b_out, ln2_gain, ln2_bias, w_up.astype(jnp.float32), b_up, w_down.astype(jnp.float32), b_down)
    output, pull = jax.vjp(partial(forward, valid_col, masked_col, validity), *params)
    grads = pull(out_grad.astype(jnp.float32))
    return (output.astype(jnp.bfloat16), grads[0], grads[1], grads[2], grads[3], grads[4], grads[5], grads[6], grads[7], grads[8], grads[9], grads[10], grads[11], grads[12], grads[13])
```

```python
import jax
import jax.numpy as jnp
from jax import lax
from jax.sharding import PartitionSpec as P

HEAD_DIM = 64
AXES = ("dp", "tp")
BF = jnp.bfloat16
F32 = jnp.float32


def layer_norm(values, gain, bias):
    center = values - jnp.mean(values, -1, keepdims=True)
    spread = jnp.mean(center * center, -1, keepdims=True)
    return center * lax.rsqrt(spread + 1e-06) * gain + bias


def exact_gelu(values):
    return jax.nn.gelu(values, approximate=False)


def outer_sum(left, right):
    return lax.dot_general(left, right, (((0,), (0,)), ((), ())), preferred_element_type=F32)


def dot_trans(left, right):
    return lax.dot_general(left, right, (((1,), (1,)), ((), ())), preferred_element_type=F32)


def dot(left, right):
    return jnp.dot(left, right, preferred_element_type=F32)


def masked_scores(query_rows, key_rows, keep_key):
    scores = jnp.einsum("qhd,khd->hqk", query_rows, key_rows, preferred_element_type=F32)
    return jnp.where(keep_key[None, None, :] > 0, scores * HEAD_DIM ** (-0.5), -1000000000.0)


def attend(packed, keep_key):
    scores = masked_scores(packed[:, 0], packed[:, 1], keep_key)
    row_max = jnp.max(scores, -1, keepdims=True)
    powered = jnp.exp(scores - row_max)
    row_sum = jnp.sum(powered, -1, keepdims=True)
    weights = (powered / row_sum).astype(BF)
    context = jnp.einsum("hqk,khd->qhd", weights, packed[:, 2], preferred_element_type=F32)
    return context.astype(BF), (row_max + jnp.log(row_sum))[..., 0]


def attend_back(packed, keep_key, log_norm, grad_ctx):
    query_rows, key_rows, value_rows = packed[:, 0], packed[:, 1], packed[:, 2]
    scale = HEAD_DIM ** (-0.5)
    weights = jnp.exp(masked_scores(query_rows, key_rows, keep_key) - log_norm[..., None])
    grad_weights = jnp.einsum("qhd,khd->hqk", grad_ctx, value_rows, preferred_element_type=F32)
    inner = jnp.sum(weights * grad_weights, -1, keepdims=True)
    grad_scores = (weights * (grad_weights - inner)).astype(BF)
    grad_query = jnp.einsum("hqk,khd->qhd", grad_scores, key_rows, preferred_element_type=F32) * scale
    grad_key = jnp.einsum("hqk,qhd->khd", grad_scores, query_rows, preferred_element_type=F32) * scale
    grad_value = jnp.einsum("hqk,qhd->khd", weights.astype(BF), grad_ctx, preferred_element_type=F32)
    return jnp.stack([grad_query, grad_key, grad_value], 1).astype(BF)


class Wires:
    def __init__(self, n_dp, n_tp):
        assert n_tp == 4 and n_dp % 8 == 0
        self.n_dp, self.n_tp = n_dp, n_tp
        every = [(d, t) for d in range(n_dp) for t in range(n_tp)]
        flat = lambda d, t: d * n_tp + t
        self.flip = {}
        bit = 1
        while bit < n_dp:
            self.flip[bit] = [(flat(d, t), flat(d ^ bit, t)) for d, t in every]
            bit *= 2
        self.tflip = {b: [(flat(d, t), flat(d, t ^ b)) for d, t in every] for b in (1, 2)}
        self.swap = [(flat(d, t), flat(d ^ 1, t ^ 1)) for d, t in every if (d ^ t) & 1]
        pull, push = [], []
        for d, t in every:
            c = d & 1
            shard = 2 * c + (t & 1)
            if t >> 1 == c:
                pull.append((flat(d, t ^ 1), flat(d, t)))
                push.append((flat(d, t), flat(d, t ^ 1)))
            else:
                pull.append((flat(d ^ 1, shard), flat(d, t)))
                push.append((flat(d, t), flat(d ^ 1, shard)))
        self.pull, self.push = pull, push
        self.away = [(flat(d, t), flat(d, t ^ 1)) for d, t in every if t >> 1 != d & 1]

    def go(self, value, perm):
        return lax.ppermute(value, AXES, perm)

    def where(self):
        d, t = lax.axis_index("dp"), lax.axis_index("tp")
        return d, t, d & 1, (d >> 1) & 3, (t >> 1) == (d & 1)


def place(pieces, quarter, axis):
    shape = list(pieces[0].shape)
    rows = shape[axis]
    shape[axis] = 4 * rows
    full = jnp.zeros(shape, pieces[0].dtype)
    for index, piece in enumerate(pieces):
        full = lax.dynamic_update_slice_in_dim(full, piece, (quarter ^ index) * rows, axis)
    return full


def spread_plane(w, mine, quarter):
    half = mine.shape[1] // 2
    rx = w.go(mine, w.flip[2])
    ry = w.go(mine, w.flip[4])
    dx = w.go(ry[:, :half], w.flip[2])
    dy = w.go(rx[:, half:], w.flip[4])
    return place([mine, rx, ry, jnp.concatenate([dx, dy], 1)], quarter, 1)


def gather_weights(w, shard):
    d, t, c, quarter, home = w.where()
    rows = shard.shape[0] // 4
    own = lax.dynamic_slice_in_dim(shard, quarter * rows, rows)
    first = w.go(own, w.pull)
    second = w.go(first, w.away)
    mine = jnp.stack([jnp.where(home, own, first), jnp.where(home, first, second)])
    return spread_plane(w, mine, quarter)


def reduce_grads(w, grads):
    d, t, c, quarter, home = w.where()
    rows = grads.shape[1] // 4
    half = rows // 2
    part = lambda i: lax.dynamic_slice_in_dim(grads, (quarter ^ i) * rows, rows, 1)
    diag = part(3)
    sx = w.go(diag[:, :half], w.flip[2])
    sy = w.go(diag[:, half:], w.flip[4])
    px, py = part(1), part(2)
    px = jnp.concatenate([px[:, :half], (px[:, half:].astype(F32) + sy.astype(F32)).astype(BF)], 1)
    py = jnp.concatenate([(py[:, :half].astype(F32) + sx.astype(F32)).astype(BF), py[:, half:]], 1)
    tx = w.go(px, w.flip[2])
    ty = w.go(py, w.flip[4])
    own = part(0).astype(F32) + tx.astype(F32) + ty.astype(F32)
    if w.n_dp > 8:
        groups = [[r + 8 * g for g in range(w.n_dp // 8)] for r in range(8)]
        own = lax.psum(own, "dp", axis_index_groups=groups)
    first, second = own[0], own[1]
    back = w.go(second.astype(BF), w.away)
    first = first + back.astype(F32)
    got = w.go(jnp.where(home, second, first).astype(BF), w.push).astype(F32)
    partial = jnp.where(home, first + got, got).astype(BF)
    mine = lax.dynamic_slice_in_dim(partial, c * half, half)
    other = lax.dynamic_slice_in_dim(partial, (1 - c) * half, half)
    mine = mine.astype(F32) + w.go(other, w.flip[1]).astype(F32)
    mine = mine.astype(BF)
    spread = spread_plane(w, mine[None], quarter)[0].reshape(4, half, -1)
    other = w.go(spread, w.flip[1])
    low = jnp.where(c == 0, spread, other)
    high = jnp.where(c == 0, other, spread)
    return jnp.stack([low, high], 1).reshape(4 * rows, -1).astype(F32)


def reduce_small(w, rows):
    bit = 1
    while bit < w.n_dp:
        rows = rows + w.go(rows, w.flip[bit])
        bit *= 2
    for b in (1, 2):
        rows = rows + w.go(rows, w.tflip[b])
    return rows


def split_bf(row):
    high = row.astype(BF)
    return high, (row - high.astype(F32)).astype(BF)


def shards(w, patches, validity, mask_pos, mask_token, ln1_gain, ln1_bias, w_qkv, b_qv, w_out,
           b_out, ln2_gain, ln2_bias, w_up, b_up, w_down, b_down, out_grad):
    d, t, c, quarter, home = w.where()
    rows, width = patches.shape
    seq = validity.shape[1]
    local = w_qkv.shape[2]
    heads = local // HEAD_DIM
    core = w.flip[1]
    both = lambda v: jnp.concatenate([v, w.go(v, core)], 0)
    swapped = ((d ^ t) & 1) == 1

    def swap(v):
        return jnp.where(swapped, w.go(v, w.swap), v)

    patches = swap(patches)
    bucket = t >> 1
    flags = jnp.stack([lax.dynamic_index_in_dim(validity, bucket, 0, False),
                       lax.dynamic_index_in_dim(mask_pos, bucket, 0, False)])
    flags = jnp.where(swapped, w.go(flags, core), flags)
    own_flags = lax.dynamic_slice_in_dim(flags, c * rows, rows, 1)
    other_flags = lax.dynamic_slice_in_dim(flags, (1 - c) * rows, rows, 1)
    keep_key = jnp.concatenate([own_flags[0], other_flags[0]])
    valid_col = own_flags[0].astype(F32)[:, None]
    masked_col = own_flags[1].astype(F32)[:, None]
    keep_token = valid_col * (1.0 - masked_col)
    swap_token = valid_col * masked_col

    wide = 3 * local
    up_hi, up_lo = split_bf(b_up)
    qv_hi, qv_lo = split_bf(jnp.pad(b_qv.reshape(-1), (0, width - 2 * local)))
    pad1 = -(wide + 4) % 128
    shard1 = jnp.concatenate([w_qkv.reshape(width, wide).T, up_hi[None], up_lo[None], qv_hi[None],
                              qv_lo[None], jnp.zeros((pad1, width), BF)])
    full1 = gather_weights(w, shard1)
    units = w_up.shape[1]
    tall = local + width + units
    pad2 = -tall % 128
    shard2 = jnp.concatenate([w_out, w_up, w_down, jnp.zeros((pad2, width), BF)])
    full2 = gather_weights(w, shard2)
    wq = full1[:, :wide]
    small = full1[:, wide:wide + 4].astype(F32)
    bias_up = (small[:, 0] + small[:, 1])
    bias_qv = (small[:, 2] + small[:, 3])[:, :2 * local].reshape(2, 2, local)
    wo = full2[:, :local]
    wu = full2[:, local:local + width]
    wd = full2[:, local + width:tall]

    block_in = keep_token * patches.astype(F32) + swap_token * mask_token[None, :]
    normed_f, ln1_pull = jax.vjp(layer_norm, block_in, ln1_gain, ln1_bias)
    normed_all = both(normed_f.astype(BF))
    slots = (0, 1)
    qkv = []
    for s in slots:
        bias = jnp.concatenate([bias_qv[s, 0], jnp.zeros((local,), F32), bias_qv[s, 1]])
        got = (dot_trans(normed_all, wq[s]) + bias[None]).astype(BF)
        qkv.append(got.reshape(seq, 3, heads, HEAD_DIM))
    attended = [attend(qkv[s], keep_key) for s in slots]
    context = [a[0].reshape(seq, local) for a in attended]
    attn_part = dot(context[0], wo[0]) + dot(context[1], wo[1])
    attn_rows = attn_part[:rows] + w.go(attn_part[rows:].astype(BF), core).astype(F32)
    residual = block_in + attn_rows + b_out[None, :]
    normed_g, ln2_pull = jax.vjp(layer_norm, residual, ln2_gain, ln2_bias)
    normed_mlp = both(normed_g.astype(BF))
    hidden, gelu_pull = [], []
    for s in slots:
        hidden_pre = dot(normed_mlp, wu[s]) + bias_up[s][None, :]
        gelu_out, pull = jax.vjp(exact_gelu, hidden_pre)
        hidden.append(gelu_out.astype(BF))
        gelu_pull.append(pull)
    mlp_part = dot(hidden[0], wd[0]) + dot(hidden[1], wd[1])
    mlp_rows = mlp_part[:rows] + w.go(mlp_part[rows:].astype(BF), core).astype(F32)
    output = (valid_col * (residual + mlp_rows + b_down[None, :])).astype(BF)
    output = swap(output)

    grad_out = valid_col * swap(out_grad).astype(F32)
    grad_b_down = jnp.sum(grad_out, 0)
    grad_all = both(grad_out.astype(BF))
    g_up, g_down, g_bup, gn2 = [], [], [], 0.0
    for s in slots:
        g_down.append(outer_sum(hidden[s], grad_all).astype(BF))
        grad_pre = gelu_pull[s](dot_trans(grad_all, wd[s]))[0].astype(BF)
        g_up.append(outer_sum(normed_mlp, grad_pre).astype(BF))
        g_bup.append(jnp.sum(grad_pre.astype(F32), 0))
        gn2 = gn2 + dot_trans(grad_pre, wu[s])
    gn2 = gn2[:rows] + w.go(gn2[rows:].astype(BF), core).astype(F32)
    grad_res_part, grad_ln2_gain, grad_ln2_bias = ln2_pull(gn2)
    grad_res = grad_out + grad_res_part
    grad_b_out = jnp.sum(grad_res, 0)
    grad_res_all = both(grad_res.astype(BF))
    g_out = [outer_sum(context[s], grad_res_all).astype(BF) for s in slots]
    zeros2 = jnp.zeros((pad2, width), BF)
    final2 = reduce_grads(w, jnp.stack(
        [jnp.concatenate([g_out[s], g_up[s], g_down[s], zeros2]) for s in slots]))
    g_qkv, gn1, g_b = [], 0.0, []
    for s in slots:
        grad_context = dot_trans(grad_res_all, wo[s]).astype(BF)
        packed = attend_back(qkv[s], keep_key, attended[s][1],
                             grad_context.reshape(seq, heads, HEAD_DIM)).reshape(seq, wide)
        g_qkv.append(outer_sum(packed, normed_all).astype(BF))
        sums = jnp.sum(packed.astype(F32), 0)
        g_b.append(jnp.pad(jnp.concatenate([sums[:local], sums[2 * local:]]), (0, width - 2 * local)))
        gn1 = gn1 + dot(packed, wq[s])
    zeros1 = jnp.zeros((pad1 + 2, width), BF)
    final1 = reduce_grads(w, jnp.stack(
        [jnp.concatenate([g_qkv[s], g_bup[s][None].astype(BF), g_b[s][None].astype(BF), zeros1])
         for s in slots]))
    gn1 = gn1[:rows] + w.go(gn1[rows:].astype(BF), core).astype(F32)
    grad_in_part, grad_ln1_gain, grad_ln1_bias = ln1_pull(gn1)
    grad_in = grad_res + grad_in_part
    grad_patches = keep_token * grad_in
    grad_mask_token = jnp.sum(swap_token * grad_in, 0)
    grad_patches = jnp.where(swapped, w.go(grad_patches.astype(BF), w.swap).astype(F32), grad_patches)
    totals = reduce_small(w, jnp.stack([grad_mask_token, grad_ln1_gain, grad_ln1_bias, grad_b_out,
                                        grad_ln2_gain, grad_ln2_bias, grad_b_down]))
    grad_w_qkv = final1[:wide].T.reshape(width, 3, local)
    grad_b_up = final1[wide]
    grad_b_qv = final1[wide + 1][:2 * local].reshape(2, local)
    grad_w_out = final2[:local]
    grad_w_up = final2[local:local + width]
    grad_w_down = final2[local + width:tall]
    return (output, grad_patches, totals[0], totals[1], totals[2], grad_w_qkv, grad_b_qv,
            grad_w_out, totals[3], totals[4], totals[5], grad_w_up, grad_b_up, grad_w_down,
            totals[6])


def solution(mesh):
    w = Wires(mesh.shape["dp"], mesh.shape["tp"])
    rows, cols = P(AXES, None), P(None, "tp")
    return jax.shard_map(
        lambda *args: shards(w, *args),
        mesh=mesh,
        in_specs=(rows, P("dp", None), P("dp", None), P(), P(), P(), P(None, None, "tp"), cols,
                  P("tp", None), P(), P(), P(), cols, P("tp"), P("tp", None), P(), rows),
        out_specs=(rows, rows, P(), P(), P(), P(None, None, "tp"), cols, P("tp", None), P(), P(),
                   P(), cols, P("tp"), P("tp", None), P()),
        check_vma=False,
    )
```

```python
import jax
import jax.numpy as jnp
from jax import lax
from jax.experimental import pallas as pl
from jax.experimental.pallas import tpu as pltpu
from jax.sharding import PartitionSpec as P

HEAD_DIM = 64
AXES = ("dp", "tp")
BF = jnp.bfloat16
F32 = jnp.float32


def layer_norm(values, gain, bias):
    center = values - jnp.mean(values, -1, keepdims=True)
    spread = jnp.mean(center * center, -1, keepdims=True)
    return center * lax.rsqrt(spread + 1e-06) * gain + bias


def exact_gelu(values):
    return jax.nn.gelu(values, approximate=False)


def outer_sum(left, right):
    return lax.dot_general(left, right, (((0,), (0,)), ((), ())), preferred_element_type=F32)


def dot_trans(left, right):
    return lax.dot_general(left, right, (((1,), (1,)), ((), ())), preferred_element_type=F32)


def dot(left, right):
    return jnp.dot(left, right, preferred_element_type=F32)


def dg(left, right, ldim, rdim):
    return lax.dot_general(left, right, (((ldim,), (rdim,)), ((), ())), preferred_element_type=F32)


def fwd_kernel(bias_ref, qkv_ref, ctx_ref, lse_ref):
    q, k, v = (qkv_ref[0, i, 0] for i in range(3))
    seq, block = q.shape[1], 512
    summed = jnp.concatenate([v, jnp.ones((16, seq), BF)], 0)

    def score(start):
        part = q[:, start:start + block] * jnp.asarray(HEAD_DIM ** (-0.5), BF)
        return dg(k, part, 0, 0) + bias_ref[...]

    starts = list(range(0, seq, block))
    scores = score(0)
    for index, start in enumerate(starts):
        later = score(starts[index + 1]) if index + 1 < len(starts) else None
        top = jnp.max(scores, 0, keepdims=True)
        powered = jnp.exp(scores - top)
        out = dg(summed, powered.astype(BF), 1, 0)
        total = out[HEAD_DIM:HEAD_DIM + 1]
        ctx_ref[0, 0, :, start:start + block] = (out[:HEAD_DIM] / total).astype(BF)
        lse_ref[0, 0, :, start:start + block] = top + jnp.log(total)
        scores = later


def bwd_kernel(bias_ref, qkv_ref, do_ref, ctx_ref, lse_ref, out_ref, dk_ref, dv_ref):
    q, k, v = (qkv_ref[0, i, 0] for i in range(3))
    seq, block = q.shape[1], 256
    do = do_ref[0, 0]
    inner = jnp.sum(do.astype(F32) * ctx_ref[0, 0].astype(F32), 0, keepdims=True)
    for start in range(0, seq, block):
        blk = slice(start, start + block)
        part = q[:, blk] * jnp.asarray(HEAD_DIM ** (-0.5), BF)
        dob = do[:, blk]
        probs = jnp.exp(dg(k, part, 0, 0) + bias_ref[...] - lse_ref[0, 0, :, blk])
        ds = (probs * (dg(v, dob, 0, 0) - inner[:, blk])).astype(BF)
        dv = dg(dob, probs.astype(BF), 1, 1)
        dk = dg(part, ds, 1, 1)
        if start:
            dk_ref[...] += dk
            dv_ref[...] += dv
        else:
            dk_ref[...] = dk
            dv_ref[...] = dv
        out_ref[0, 0, 0, :, blk] = (dg(k, ds, 1, 0) * HEAD_DIM ** (-0.5)).astype(BF)
    out_ref[0, 1, 0] = dk_ref[...].astype(BF)
    out_ref[0, 2, 0] = dv_ref[...].astype(BF)


def head_specs(heads, seq):
    col = pl.BlockSpec((seq, 1), lambda i: (0, 0))
    tri = pl.BlockSpec((1, 3, 1, HEAD_DIM, seq), lambda i: (i // heads, 0, i % heads, 0, 0))
    one = pl.BlockSpec((1, 1, HEAD_DIM, seq), lambda i: (i // heads, i % heads, 0, 0))
    row = pl.BlockSpec((1, 1, 1, seq), lambda i: (i // heads, i % heads, 0, 0))
    return col, tri, one, row


def attend(bias, qkv):
    slots, _, heads, _, seq = qkv.shape
    col, tri, one, row = head_specs(heads, seq)
    pairs = slots * heads * seq * seq
    return pl.pallas_call(
        fwd_kernel, grid=(slots * heads,), in_specs=[col, tri], out_specs=[one, row],
        out_shape=[jax.ShapeDtypeStruct((slots, heads, HEAD_DIM, seq), BF),
                   jax.ShapeDtypeStruct((slots, heads, 1, seq), F32)],
        cost_estimate=pl.CostEstimate(flops=pairs * 4 * HEAD_DIM, bytes_accessed=qkv.size * 3,
                                      transcendentals=pairs))(bias, qkv)


def attend_back(bias, qkv, do, ctx, lse):
    slots, _, heads, _, seq = qkv.shape
    col, tri, one, row = head_specs(heads, seq)
    pairs = slots * heads * seq * seq
    return pl.pallas_call(
        bwd_kernel, grid=(slots * heads,), in_specs=[col, tri, one, one, row], out_specs=tri,
        out_shape=jax.ShapeDtypeStruct(qkv.shape, BF),
        scratch_shapes=[pltpu.VMEM((HEAD_DIM, seq), F32)] * 2,
        cost_estimate=pl.CostEstimate(flops=pairs * 10 * HEAD_DIM, bytes_accessed=qkv.size * 6,
                                      transcendentals=pairs))(bias, qkv, do, ctx, lse)


class Wires:
    def __init__(self, n_dp, n_tp):
        assert n_tp == 4 and n_dp % 8 == 0
        self.n_dp, self.n_tp = n_dp, n_tp
        every = [(d, t) for d in range(n_dp) for t in range(n_tp)]
        flat = lambda d, t: d * n_tp + t
        self.flip = {}
        bit = 1
        while bit < n_dp:
            self.flip[bit] = [(flat(d, t), flat(d ^ bit, t)) for d, t in every]
            bit *= 2
        self.tflip = {b: [(flat(d, t), flat(d, t ^ b)) for d, t in every] for b in (1, 2)}
        self.swap = [(flat(d, t), flat(d ^ 1, t ^ 1)) for d, t in every if (d ^ t) & 1]
        pull, push = [], []
        for d, t in every:
            c = d & 1
            shard = 2 * c + (t & 1)
            if t >> 1 == c:
                pull.append((flat(d, t ^ 1), flat(d, t)))
                push.append((flat(d, t), flat(d, t ^ 1)))
            else:
                pull.append((flat(d ^ 1, shard), flat(d, t)))
                push.append((flat(d, t), flat(d ^ 1, shard)))
        self.pull, self.push = pull, push
        self.away = [(flat(d, t), flat(d, t ^ 1)) for d, t in every if t >> 1 != d & 1]

    def go(self, value, perm):
        return lax.ppermute(value, AXES, perm)

    def where(self):
        d, t = lax.axis_index("dp"), lax.axis_index("tp")
        return d, t, d & 1, (d >> 1) & 3, (t >> 1) == (d & 1)


def place(pieces, quarter, axis):
    shape = list(pieces[0].shape)
    rows = shape[axis]
    shape[axis] = 4 * rows
    full = jnp.zeros(shape, pieces[0].dtype)
    for index, piece in enumerate(pieces):
        full = lax.dynamic_update_slice_in_dim(full, piece, (quarter ^ index) * rows, axis)
    return full


def spread_plane(w, mine, quarter):
    half = mine.shape[1] // 2
    rx = w.go(mine, w.flip[2])
    ry = w.go(mine, w.flip[4])
    dx = w.go(ry[:, :half], w.flip[2])
    dy = w.go(rx[:, half:], w.flip[4])
    return place([mine, rx, ry, jnp.concatenate([dx, dy], 1)], quarter, 1)


def gather_weights(w, shard):
    d, t, c, quarter, home = w.where()
    rows = shard.shape[0] // 4
    own = lax.dynamic_slice_in_dim(shard, quarter * rows, rows)
    first = w.go(own, w.pull)
    second = w.go(first, w.away)
    mine = jnp.stack([jnp.where(home, own, first), jnp.where(home, first, second)])
    return spread_plane(w, mine, quarter)


def reduce_grads(w, grads):
    d, t, c, quarter, home = w.where()
    rows = grads.shape[1] // 4
    half = rows // 2
    part = lambda i: lax.dynamic_slice_in_dim(grads, (quarter ^ i) * rows, rows, 1)
    diag = part(3)
    sx = w.go(diag[:, :half], w.flip[2])
    sy = w.go(diag[:, half:], w.flip[4])
    px, py = part(1), part(2)
    px = jnp.concatenate([px[:, :half], (px[:, half:].astype(F32) + sy.astype(F32)).astype(BF)], 1)
    py = jnp.concatenate([(py[:, :half].astype(F32) + sx.astype(F32)).astype(BF), py[:, half:]], 1)
    tx = w.go(px, w.flip[2])
    ty = w.go(py, w.flip[4])
    own = part(0).astype(F32) + tx.astype(F32) + ty.astype(F32)
    if w.n_dp > 8:
        groups = [[r + 8 * g for g in range(w.n_dp // 8)] for r in range(8)]
        own = lax.psum(own, "dp", axis_index_groups=groups)
    first, second = own[0], own[1]
    back = w.go(second.astype(BF), w.away)
    first = first + back.astype(F32)
    got = w.go(jnp.where(home, second, first).astype(BF), w.push).astype(F32)
    partial = jnp.where(home, first + got, got).astype(BF)
    mine = lax.dynamic_slice_in_dim(partial, c * half, half)
    other = lax.dynamic_slice_in_dim(partial, (1 - c) * half, half)
    mine = mine.astype(F32) + w.go(other, w.flip[1]).astype(F32)
    mine = mine.astype(BF)
    spread = spread_plane(w, mine[None], quarter)[0].reshape(4, half, -1)
    other = w.go(spread, w.flip[1])
    low = jnp.where(c == 0, spread, other)
    high = jnp.where(c == 0, other, spread)
    return jnp.stack([low, high], 1).reshape(4 * rows, -1).astype(F32)


def reduce_small(w, rows):
    bit = 1
    while bit < w.n_dp:
        rows = rows + w.go(rows, w.flip[bit])
        bit *= 2
    for b in (1, 2):
        rows = rows + w.go(rows, w.tflip[b])
    return rows


def split_bf(row):
    high = row.astype(BF)
    return high, (row - high.astype(F32)).astype(BF)


def shards(w, patches, validity, mask_pos, mask_token, ln1_gain, ln1_bias, w_qkv, b_qv, w_out,
           b_out, ln2_gain, ln2_bias, w_up, b_up, w_down, b_down, out_grad):
    d, t, c, quarter, home = w.where()
    rows, width = patches.shape
    seq = validity.shape[1]
    local = w_qkv.shape[2]
    heads = local // HEAD_DIM
    core = w.flip[1]
    both = lambda v: jnp.concatenate([v, w.go(v, core)], 0)
    swapped = ((d ^ t) & 1) == 1

    def swap(v):
        return jnp.where(swapped, w.go(v, w.swap), v)

    patches = swap(patches)
    bucket = t >> 1
    flags = jnp.stack([lax.dynamic_index_in_dim(validity, bucket, 0, False),
                       lax.dynamic_index_in_dim(mask_pos, bucket, 0, False)])
    flags = jnp.where(swapped, w.go(flags, core), flags)
    own_flags = lax.dynamic_slice_in_dim(flags, c * rows, rows, 1)
    other_flags = lax.dynamic_slice_in_dim(flags, (1 - c) * rows, rows, 1)
    keep_key = jnp.concatenate([own_flags[0], other_flags[0]])
    valid_col = own_flags[0].astype(F32)[:, None]
    masked_col = own_flags[1].astype(F32)[:, None]
    keep_token = valid_col * (1.0 - masked_col)
    swap_token = valid_col * masked_col

    wide = 3 * local
    up_hi, up_lo = split_bf(b_up)
    qv_hi, qv_lo = split_bf(jnp.pad(b_qv.reshape(-1), (0, width - 2 * local)))
    pad1 = -(wide + 4) % 128
    shard1 = jnp.concatenate([w_qkv.reshape(width, wide).T, up_hi[None], up_lo[None], qv_hi[None],
                              qv_lo[None], jnp.zeros((pad1, width), BF)])
    full1 = gather_weights(w, shard1)
    units = w_up.shape[1]
    tall = local + width + units
    pad2 = -tall % 128
    shard2 = jnp.concatenate([w_out, w_up, w_down, jnp.zeros((pad2, width), BF)])
    full2 = gather_weights(w, shard2)
    wq = full1[:, :wide]
    small = full1[:, wide:wide + 4].astype(F32)
    bias_up = (small[:, 0] + small[:, 1])
    bias_qv = (small[:, 2] + small[:, 3])[:, :2 * local].reshape(2, 2, local)
    wo = full2[:, :local]
    wu = full2[:, local:local + width]
    wd = full2[:, local + width:tall]

    block_in = keep_token * patches.astype(F32) + swap_token * mask_token[None, :]
    normed_f, ln1_pull = jax.vjp(layer_norm, block_in, ln1_gain, ln1_bias)
    normed_all = both(normed_f.astype(BF))
    slots = (0, 1)
    qkv = []
    for s in slots:
        bias = jnp.concatenate([bias_qv[s, 0], jnp.zeros((local,), F32), bias_qv[s, 1]])
        qkv.append((dot_trans(wq[s], normed_all) + bias[:, None]).astype(BF))
    qkv = jnp.stack(qkv).reshape(2, 3, heads, HEAD_DIM, seq)
    key_bias = jnp.where(keep_key > 0, 0.0, -1000000000.0)[:, None]
    context, log_norm = attend(key_bias, qkv)
    context_rows = context.reshape(2 * local, seq)
    wo_rows = wo.reshape(2 * local, width)
    attn_part = outer_sum(context_rows, wo_rows)
    attn_rows = attn_part[:rows] + w.go(attn_part[rows:].astype(BF), core).astype(F32)
    residual = block_in + attn_rows + b_out[None, :]
    normed_g, ln2_pull = jax.vjp(layer_norm, residual, ln2_gain, ln2_bias)
    normed_mlp = both(normed_g.astype(BF))
    hidden, gelu_pull = [], []
    for s in slots:
        hidden_pre = dot(normed_mlp, wu[s]) + bias_up[s][None, :]
        gelu_out, pull = jax.vjp(exact_gelu, hidden_pre)
        hidden.append(gelu_out.astype(BF))
        gelu_pull.append(pull)
    mlp_part = dot(hidden[0], wd[0]) + dot(hidden[1], wd[1])
    mlp_rows = mlp_part[:rows] + w.go(mlp_part[rows:].astype(BF), core).astype(F32)
    output = (valid_col * (residual + mlp_rows + b_down[None, :])).astype(BF)
    output = swap(output)

    grad_out = valid_col * swap(out_grad).astype(F32)
    grad_b_down = jnp.sum(grad_out, 0)
    grad_all = both(grad_out.astype(BF))
    g_up, g_down, g_bup, gn2 = [], [], [], 0.0
    for s in slots:
        g_down.append(outer_sum(hidden[s], grad_all).astype(BF))
        grad_pre = gelu_pull[s](dot_trans(grad_all, wd[s]))[0].astype(BF)
        g_up.append(outer_sum(normed_mlp, grad_pre).astype(BF))
        g_bup.append(jnp.sum(grad_pre.astype(F32), 0))
        gn2 = gn2 + dot_trans(grad_pre, wu[s])
    gn2 = gn2[:rows] + w.go(gn2[rows:].astype(BF), core).astype(F32)
    grad_res_part, grad_ln2_gain, grad_ln2_bias = ln2_pull(gn2)
    grad_res = grad_out + grad_res_part
    grad_b_out = jnp.sum(grad_res, 0)
    grad_res_all = both(grad_res.astype(BF))
    g_out = dot(context_rows, grad_res_all).astype(BF).reshape(2, local, width)
    zeros2 = jnp.zeros((pad2, width), BF)
    final2 = reduce_grads(w, jnp.stack(
        [jnp.concatenate([g_out[s], g_up[s], g_down[s], zeros2]) for s in slots]))
    g_qkv, gn1, g_b = [], 0.0, []
    grad_context = dot_trans(wo_rows, grad_res_all).astype(BF)
    grad_qkv = attend_back(key_bias, qkv, grad_context.reshape(context.shape), context, log_norm)
    for s in slots:
        packed = grad_qkv[s].reshape(wide, seq)
        g_qkv.append(dot(packed, normed_all).astype(BF))
        sums = jnp.sum(packed.astype(F32), 1)
        g_b.append(jnp.pad(jnp.concatenate([sums[:local], sums[2 * local:]]), (0, width - 2 * local)))
        gn1 = gn1 + outer_sum(packed, wq[s])
    zeros1 = jnp.zeros((pad1 + 2, width), BF)
    final1 = reduce_grads(w, jnp.stack(
        [jnp.concatenate([g_qkv[s], g_bup[s][None].astype(BF), g_b[s][None].astype(BF), zeros1])
         for s in slots]))
    gn1 = gn1[:rows] + w.go(gn1[rows:].astype(BF), core).astype(F32)
    grad_in_part, grad_ln1_gain, grad_ln1_bias = ln1_pull(gn1)
    grad_in = grad_res + grad_in_part
    grad_patches = keep_token * grad_in
    grad_mask_token = jnp.sum(swap_token * grad_in, 0)
    grad_patches = jnp.where(swapped, w.go(grad_patches.astype(BF), w.swap).astype(F32), grad_patches)
    totals = reduce_small(w, jnp.stack([grad_mask_token, grad_ln1_gain, grad_ln1_bias, grad_b_out,
                                        grad_ln2_gain, grad_ln2_bias, grad_b_down]))
    grad_w_qkv = final1[:wide].T.reshape(width, 3, local)
    grad_b_up = final1[wide]
    grad_b_qv = final1[wide + 1][:2 * local].reshape(2, local)
    grad_w_out = final2[:local]
    grad_w_up = final2[local:local + width]
    grad_w_down = final2[local + width:tall]
    return (output, grad_patches, totals[0], totals[1], totals[2], grad_w_qkv, grad_b_qv,
            grad_w_out, totals[3], totals[4], totals[5], grad_w_up, grad_b_up, grad_w_down,
            totals[6])


def solution(mesh):
    w = Wires(mesh.shape["dp"], mesh.shape["tp"])
    rows, cols = P(AXES, None), P(None, "tp")
    return jax.shard_map(
        lambda *args: shards(w, *args),
        mesh=mesh,
        in_specs=(rows, P("dp", None), P("dp", None), P(), P(), P(), P(None, None, "tp"), cols,
                  P("tp", None), P(), P(), P(), cols, P("tp"), P("tp", None), P(), rows),
        out_specs=(rows, rows, P(), P(), P(), P(None, None, "tp"), cols, P("tp", None), P(), P(),
                   P(), cols, P("tp"), P("tp", None), P()),
        check_vma=False,
    )
```

```python
import jax
import jax.numpy as jnp
from jax import lax
from jax.experimental import pallas as pl
from jax.experimental.pallas import tpu as pltpu
from jax.sharding import PartitionSpec as P

HEAD_DIM = 64
GAP = 4
PIECES = 8
CHUNK = 16
AXES = ("dp", "tp")
BF = jnp.bfloat16
F32 = jnp.float32


def layer_norm(values, gain, bias):
    center = values - jnp.mean(values, -1, keepdims=True)
    spread = jnp.mean(center * center, -1, keepdims=True)
    return center * lax.rsqrt(spread + 1e-06) * gain + bias


def exact_gelu(values):
    return jax.nn.gelu(values, approximate=False)


def outer_sum(left, right):
    return lax.dot_general(left, right, (((0,), (0,)), ((), ())), preferred_element_type=F32)


def dot_trans(left, right):
    return lax.dot_general(left, right, (((1,), (1,)), ((), ())), preferred_element_type=F32)


def dot(left, right):
    return jnp.dot(left, right, preferred_element_type=F32)


def dg(left, right, ldim, rdim):
    return lax.dot_general(left, right, (((ldim,), (rdim,)), ((), ())), preferred_element_type=F32)


def first_row(block):
    return jnp.where(lax.broadcasted_iota(jnp.int32, (16, block), 0) < 1, 1.0, 0.0).astype(BF)


def head_specs(heads, seq, parts):
    head = lambda i: (i // parts // heads, i // parts % heads)
    col = pl.BlockSpec((16, seq), lambda i: (0, 0))
    tri = pl.BlockSpec((1, 3, 1, HEAD_DIM, seq), lambda i: (head(i)[0], 0, head(i)[1], 0, 0))
    one = pl.BlockSpec((1, 1, HEAD_DIM, seq), lambda i: head(i) + (0, 0))
    row = pl.BlockSpec((1, 1, 1, seq), lambda i: head(i) + (0, 0))
    return col, tri, one, row


class Me:
    def __init__(self):
        d, t = lax.axis_index("dp"), lax.axis_index("tp")
        c, qx, qy = d % 2, (d // 2) % 2, (d // 4) % 2
        self.c = c
        self.home = (t // 2 + c + 1) % 2
        self.swapped = (d + t) % 2
        self.core = {"dp": d + 1 - 2 * c, "tp": t}
        self.x = {"dp": d + 2 - 4 * qx, "tp": t}
        self.y = {"dp": d + 4 - 8 * qy, "tp": t}
        self.near = {"dp": d, "tp": t + 1 - 2 * (t % 2)}
        self.far = {"dp": d + 1 - 2 * c, "tp": 2 * c + t % 2}
        self.cross = {"dp": d + 1 - 2 * c, "tp": t + 1 - 2 * (t % 2)}
        self.two = {"dp": d, "tp": t + 2 - 4 * (t // 2)}
        self.q = [qx + 2 * qy, 1 - qx + 2 * qy, qx + 2 * (1 - qy), 1 - qx + 2 * (1 - qy)]

    def greet(self, swap=True, two=False):
        barrier = pltpu.get_barrier_semaphore()
        others = [self.core, self.x, self.y, self.near] + ([self.two] if two else [])
        for other in others:
            pl.semaphore_signal(barrier, inc=1, device_id=other, device_id_type=MESH)

        @pl.when(self.home == 0)
        def _():
            pl.semaphore_signal(barrier, inc=1, device_id=self.far, device_id_type=MESH)

        if swap:
            @pl.when(self.swapped == 1)
            def _():
                pl.semaphore_signal(barrier, inc=1, device_id=self.cross, device_id_type=MESH)

        extra = self.swapped if swap else 0
        pl.semaphore_wait(barrier, len(others) + 1 - self.home + extra)


class Cross:
    @staticmethod
    def sems():
        return [pltpu.SemaphoreType.DMA((PIECES,)), pltpu.SemaphoreType.DMA((PIECES,))]

    def __init__(self, me, src, dst, send, recv):
        self.me, self.src, self.dst, self.send, self.recv = me, src, dst, send, recv

    def copy(self, i):
        return pltpu.make_async_remote_copy(
            src_ref=self.src.at[i], dst_ref=self.dst.at[i], send_sem=self.send.at[i],
            recv_sem=self.recv.at[i], device_id=self.me.cross, device_id_type=MESH)

    def keep(self, i):
        return pltpu.make_async_copy(self.src.at[i], self.dst.at[i], self.recv.at[i])

    def start(self, i):
        @pl.when(self.me.swapped == 1)
        def _():
            self.copy(i).start()

        @pl.when(self.me.swapped == 0)
        def _():
            self.keep(i).start()

    def wait(self, i):
        @pl.when(self.me.swapped == 1)
        def _():
            self.copy(i).wait_recv()

        @pl.when(self.me.swapped == 0)
        def _():
            self.keep(i).wait()

    def drain(self):
        @pl.when(self.me.swapped == 1)
        def _():
            for i in range(PIECES):
                self.copy(i).wait_send()


class Gather:
    STAGES = 4
    SEMS = 6

    def __init__(self, me, srcs, full, send, recv, local):
        self.me, self.srcs, self.full, self.send, self.recv = me, srcs, full, send, recv
        self.local = local
        self.n = full.shape[2]
        self.spans = spans(srcs)

    def keep_own(self, act):
        @pl.when(self.me.home == 1)
        def _():
            for i, (src, (low, high)) in enumerate(zip(self.srcs, self.spans)):
                act(pltpu.make_async_copy(src, self.full.at[0, :, pl.ds(low, high - low)],
                                          self.local.at[i]))

    def copy(self, kind, n, src, dst, device):
        return pltpu.make_async_remote_copy(
            src_ref=src, dst_ref=dst, send_sem=self.send.at[kind, n],
            recv_sem=self.recv.at[kind, n], device_id=device, device_id_type=MESH)

    def pull(self, n, home, src=None):
        me, q = self.me, self.me.q[0]
        slot = 1 if home else 0
        src = self.full.at[slot, q, n] if src is None else src
        return self.copy(0, n, src, self.full.at[slot, q, n], me.near if home else me.far)

    def relay(self, n):
        q = self.me.q[0]
        return self.copy(1, n, self.full.at[0, q, n], self.full.at[1, q, n], self.me.near)

    def plane(self, n, home):
        q, first = self.me.q[0], (1 if home else 0)
        part = self.full.at[pl.ds(first, 2 - first), q, n]
        return [self.copy(2, n, part, part, self.me.x), self.copy(3, n, part, part, self.me.y)]

    def diag(self, n, slot, through_x):
        if through_x:
            part = self.full.at[slot, self.me.q[2], n]
            return self.copy(4, n, part, part, self.me.x)
        part = self.full.at[slot, self.me.q[1], n]
        return self.copy(5, n, part, part, self.me.y)

    def diags(self, n, home, act):
        if home:
            @pl.when(n % 2 == 0)
            def _():
                act(self.diag(n, 1, True))

            @pl.when(n % 2 == 1)
            def _():
                act(self.diag(n, 1, False))
        else:
            act(self.diag(n, 0, True))
            act(self.diag(n, 1, False))

    def sides(self, body):
        @pl.when(self.me.home == 1)
        def _():
            body(True)

        @pl.when(self.me.home == 0)
        def _():
            body(False)

    def start(self, n):
        @pl.when(n < self.n)
        def _():
            for src, (low, high) in zip(self.srcs, self.spans):
                @pl.when(jnp.logical_and(n >= low, n < high))
                def _(src=src, low=low):
                    part = src.at[self.me.q[0], n - low]
                    self.sides(lambda home: self.pull(n, home, part).start())

    def prologue(self):
        self.start(jnp.int32(0))
        self.start(jnp.int32(1))

    def tick(self, step):
        def stage(n, body):
            @pl.when(jnp.logical_and(n >= 0, n < self.n))
            def _():
                body(n)

        def four(n):
            self.sides(lambda home: self.diags(n, home, lambda c: c.wait_recv()))

        def three(n):
            def side(home):
                for c in self.plane(n, home):
                    c.wait_recv()
                self.diags(n, home, lambda c: c.start())
            self.sides(side)

        def two(n):
            def side(home):
                if not home:
                    self.relay(n).wait_recv()
                for c in self.plane(n, home):
                    c.start()
            self.sides(side)

        def one(n):
            def side(home):
                self.pull(n, home).wait_recv()
                if not home:
                    self.relay(n).start()
            self.sides(side)

        for index, body in reversed(list(enumerate([one, two, three, four]))):
            stage(step - 1 - GAP * index, body)
        self.start(step + 2)

    @property
    def ticks(self):
        return self.n + 1 + GAP * (self.STAGES - 1)

    def finish(self):
        def drain(n, carry):
            def side(home):
                self.pull(n, home).wait_send()
                if not home:
                    self.relay(n).wait_send()
                for c in self.plane(n, home):
                    c.wait_send()
                self.diags(n, home, lambda c: c.wait_send())
            self.sides(side)
            return carry
        lax.fori_loop(0, self.n, drain, 0)

    def write(self, outs, act):
        for i, (out, (low, high)) in enumerate(zip(outs, self.spans)):
            act(pltpu.make_async_copy(self.full.at[:, :, pl.ds(low, high - low)], out,
                                      self.local.at[i]))


class Reduce:
    STAGES = 8
    SEMS = 11

    @staticmethod
    def scratch(n, rows, cols):
        piece = (rows, cols)
        return [
            pltpu.VMEM((2, 4, n) + piece, BF), pltpu.VMEM((n,) + piece, BF),
            pltpu.VMEM((n,) + piece, BF), pltpu.VMEM((2, n) + piece, BF),
            pltpu.VMEM((2, n) + piece, BF), pltpu.VMEM((n,) + piece, BF),
            pltpu.VMEM((n,) + piece, BF), pltpu.VMEM((n,) + piece, BF),
            pltpu.VMEM((n,) + piece, BF), pltpu.VMEM((n,) + piece, F32),
            pltpu.VMEM((4, n) + piece, BF),
            pltpu.SemaphoreType.DMA((Reduce.SEMS, n)), pltpu.SemaphoreType.DMA((Reduce.SEMS, n)),
            pltpu.SemaphoreType.DMA((8,)),
        ]

    def __init__(self, me, refs):
        (self.g, self.ax, self.by, self.tx, self.ty, self.back, self.got, self.give, self.take,
         self.acc, self.fin, self.send, self.recv, self.local) = refs
        self.me = me
        self.n = self.g.shape[2]

    def copy(self, kind, n, src, dst, device):
        return pltpu.make_async_remote_copy(
            src_ref=src, dst_ref=dst, send_sem=self.send.at[kind, n],
            recv_sem=self.recv.at[kind, n], device_id=device, device_id_type=MESH)

    def corner(self, n):
        q = self.me.q[3]
        return [self.copy(0, n, self.g.at[0, q, n], self.ax.at[n], self.me.x),
                self.copy(1, n, self.g.at[1, q, n], self.by.at[n], self.me.y)]

    def side(self, n):
        q = self.me.q
        return [self.copy(2, n, self.g.at[:, q[1], n], self.tx.at[:, n], self.me.x),
                self.copy(3, n, self.g.at[:, q[2], n], self.ty.at[:, n], self.me.y)]

    def second(self, n):
        return self.copy(4, n, self.g.at[1, self.me.q[0], n], self.back.at[n], self.me.near)

    def push(self, n, home):
        q = self.me.q[0]
        if home:
            return self.copy(5, n, self.g.at[1, q, n], self.got.at[n], self.me.near)
        return self.copy(5, n, self.g.at[0, q, n], self.got.at[n], self.me.far)

    def pair(self, n):
        return self.copy(6, n, self.give.at[n], self.take.at[n], self.me.core)

    def spread(self, n):
        part = self.fin.at[self.me.q[0], n]
        return [self.copy(7, n, part, part, self.me.x), self.copy(8, n, part, part, self.me.y)]

    def diag(self, n, act):
        @pl.when(n // 2 % 2 == 0)
        def _():
            part = self.fin.at[self.me.q[2], n]
            act(self.copy(9, n, part, part, self.me.x))

        @pl.when(n // 2 % 2 == 1)
        def _():
            part = self.fin.at[self.me.q[1], n]
            act(self.copy(9, n, part, part, self.me.y))

    def share(self, n):
        part = self.fin.at[:, n]
        return self.copy(10, n, part, part, self.me.core)

    def owner(self, n, body):
        pl.when((n + self.me.c) % 2 == 0)(body)

    def helper(self, n, body):
        pl.when((n + self.me.c) % 2 == 1)(body)

    def start(self, n):
        @pl.when(n < self.n)
        def _():
            for c in self.corner(n):
                c.start()

    def load(self, srcs, act):
        index, low = 0, 0
        for src in srcs:
            pair = isinstance(src, tuple)
            count = (src[0] if pair else src).shape[1 if pair else 2]
            for slot in ((0, 1) if pair else (None,)):
                part = self.g.at[slot if pair else slice(None), :, pl.ds(low, count)]
                act(pltpu.make_async_copy(src[slot] if pair else src, part, self.local.at[index]))
                index += 1
            low += count

    def prologue(self):
        self.start(jnp.int32(0))
        self.start(jnp.int32(1))

    def tick(self, step):
        me, g, acc = self.me, self.g, self.acc
        q, c = me.q, me.c
        home_f = me.home.astype(F32)

        def stage(n, body):
            @pl.when(jnp.logical_and(n >= 0, n < self.n))
            def _():
                body(n)

        def away(body):
            pl.when(me.home == 0)(body)

        def at_home(body):
            pl.when(me.home == 1)(body)

        def eight(n):
            self.helper(n, lambda: self.share(n).wait_recv())

        def seven(n):
            def own():
                self.diag(n, lambda cp: cp.wait_recv())
                self.share(n).start()
            self.owner(n, own)

        def six(n):
            def own():
                for cp in self.spread(n):
                    cp.wait_recv()
                self.diag(n, lambda cp: cp.start())
            self.owner(n, own)

        def five(n):
            def own():
                self.pair(n).wait_recv()
                self.fin[q[0], n] = (acc[n] + self.take[n].astype(F32)).astype(BF)
                for cp in self.spread(n):
                    cp.start()
            self.owner(n, own)

        def four(n):
            at_home(lambda: self.push(n, True).wait_recv())
            away(lambda: self.push(n, False).wait_recv())
            total = acc[n] * home_f + self.got[n].astype(F32)

            def own():
                acc[n] = total

            def help_out():
                self.give[n] = total.astype(BF)
                self.pair(n).start()
            self.owner(n, own)
            self.helper(n, help_out)

        def three(n):
            def side():
                self.second(n).wait_recv()
                g[0, q[0], n] = (acc[n] + self.back[n].astype(F32)).astype(BF)
                self.push(n, False).start()
            away(side)

        def two(n):
            for cp in self.side(n):
                cp.wait_recv()
            g[1, q[0], n] = (g[1, q[0], n].astype(F32) + self.tx[1, n].astype(F32)
                             + self.ty[1, n].astype(F32)).astype(BF)
            away(lambda: self.second(n).start())
            at_home(lambda: self.push(n, True).start())
            acc[n] = (g[0, q[0], n].astype(F32) + self.tx[0, n].astype(F32)
                      + self.ty[0, n].astype(F32))

        def one(n):
            for cp in self.corner(n):
                cp.wait_recv()
            g[1, q[1], n] = (g[1, q[1], n].astype(F32) + self.by[n].astype(F32)).astype(BF)
            g[0, q[2], n] = (g[0, q[2], n].astype(F32) + self.ax[n].astype(F32)).astype(BF)
            for cp in self.side(n):
                cp.start()

        bodies = [one, two, three, four, five, six, seven, eight]
        for index in reversed(range(8)):
            stage(step - 1 - GAP * index, bodies[index])
        self.start(step + 2)

    @property
    def ticks(self):
        return self.n + 1 + GAP * (self.STAGES - 1)

    def finish(self, outs):
        def drain(n, carry):
            for cp in self.corner(n) + self.side(n):
                cp.wait_send()

            @pl.when(self.me.home == 1)
            def _():
                self.push(n, True).wait_send()

            @pl.when(self.me.home == 0)
            def _():
                self.second(n).wait_send()
                self.push(n, False).wait_send()

            def own():
                for cp in self.spread(n) + [self.share(n)]:
                    cp.wait_send()
                self.diag(n, lambda cp: cp.wait_send())
            self.owner(n, own)
            self.helper(n, lambda: self.pair(n).wait_send())
            return carry
        lax.fori_loop(0, self.n, drain, 0)
        copies, low = [], 0
        for i, out in enumerate(outs):
            count = out.shape[1]
            copies.append(pltpu.make_async_copy(self.fin.at[:, pl.ds(low, count)], out,
                                                self.local.at[i]))
            low += count
        for cp in copies:
            cp.start()
        for cp in copies:
            cp.wait()


def spans(srcs):
    result, low = [], 0
    for src in srcs:
        result.append((low, low + src.shape[1]))
        low += src.shape[1]
    return result


MESH = pl.DeviceIdType.MESH
COMM = dict(has_side_effects=True, vmem_limit_bytes=60 * 1024 * 1024)
ANY = pl.BlockSpec(memory_space=pl.ANY)


def front(patches, shard, keep, swap, vectors, small):
    n, rows, cols = shard.shape[1:]
    piece = patches.shape[1]
    wide = 4 * n * rows
    third = wide // 3
    seq = 2 * PIECES * piece

    def kernel(x_ref, src_ref, keep_ref, swap_ref, vec_ref, small_ref,
               x_out, full_out, normed_out, small_out, qkv_ref,
               x_buf, normed, small_buf, full, send, recv, local, x_send, x_recv, n_send, n_recv,
               b_send, b_recv):
        me = Me()
        gather = Gather(me, [src_ref], full, send, recv, local)
        cross = Cross(me, x_ref, x_buf, x_send, x_recv)

        def hand(i):
            return pltpu.make_async_remote_copy(
                src_ref=normed.at[0, i], dst_ref=normed.at[1, i], send_sem=n_send.at[i],
                recv_sem=n_recv.at[i], device_id=me.core, device_id_type=MESH)

        def bias_pull(home):
            return pltpu.make_async_remote_copy(
                src_ref=small_ref, dst_ref=small_buf.at[1 if home else 0], send_sem=b_send.at[0],
                recv_sem=b_recv.at[0], device_id=me.near if home else me.far, device_id_type=MESH)

        bias_relay = pltpu.make_async_remote_copy(
            src_ref=small_buf.at[0], dst_ref=small_buf.at[1], send_sem=b_send.at[1],
            recv_sem=b_recv.at[1], device_id=me.near, device_id_type=MESH)
        bias_keep = pltpu.make_async_copy(small_ref, small_buf.at[0], local.at[1])

        def home(body):
            pl.when(me.home == 1)(body)

        def away(body):
            pl.when(me.home == 0)(body)

        me.greet()
        gather.keep_own(lambda cp: cp.start())
        home(lambda: bias_keep.start())
        home(lambda: bias_pull(True).start())
        away(lambda: bias_pull(False).start())
        gather.prologue()
        cross.start(0)
        cross.start(1)
        gather.keep_own(lambda cp: cp.wait())

        def norm(i):
            at = pl.ds(pl.multiple_of(i * piece, piece), piece)
            value = (keep_ref[at, :] * x_buf[i].astype(F32)
                     + swap_ref[at, :] * vec_ref[0:1, :])
            center = value - jnp.mean(value, -1, keepdims=True)
            spread = jnp.mean(center * center, -1, keepdims=True)
            out = center * lax.rsqrt(spread + 1e-06) * vec_ref[1:2, :] + vec_ref[2:3, :]
            normed[0, i] = out.astype(BF)

        def step(index, carry):
            gather.tick(index)

            @pl.when(index < PIECES - 2)
            def _():
                cross.start(index + 2)

            @pl.when(jnp.logical_and(index >= 1, index < PIECES + 1))
            def _():
                cross.wait(index - 1)
                norm(index - 1)
                hand(index - 1).start()

            @pl.when(index == 4)
            def _():
                def relay():
                    bias_pull(False).wait_recv()
                    bias_relay.start()
                away(relay)
            return carry
        lax.fori_loop(0, max(gather.ticks, PIECES + 1), step, 0)
        gather.write([full_out], lambda cp: cp.start())
        for i in range(PIECES):
            hand(i).wait_recv()

        def own_bias():
            bias_keep.wait()
            bias_pull(True).wait_recv()
        home(own_bias)
        away(lambda: bias_relay.wait_recv())
        rows_all = normed[...].reshape(seq, cols)
        ones = jnp.where(lax.broadcasted_iota(jnp.int32, (16, seq), 0) < 2, 1.0, 0.0).astype(BF)
        for slot in range(2):
            line = small_buf[slot, 1:2, :]
            high = line.astype(BF)
            low = (line - high.astype(F32)).astype(BF)
            pair = jnp.concatenate([high, low, jnp.zeros((14, cols), BF)], 0)[:, :wide]
            weights = full[slot].reshape(wide, cols)
            for part in range(3):
                at = slice(part * third, part * third + third)
                out = dg(weights[at], rows_all, 1, 1) + dg(pair[:, at], ones, 0, 0)
                qkv_ref[slot, at] = out.astype(BF)
        x_copy = pltpu.make_async_copy(x_buf, x_out, local.at[1])
        n_copy = pltpu.make_async_copy(normed, normed_out, local.at[2])
        b_copy = pltpu.make_async_copy(small_buf, small_out, local.at[3])
        for cp in (x_copy, n_copy, b_copy):
            cp.start()
        cross.drain()
        for i in range(PIECES):
            hand(i).wait_send()
        home(lambda: bias_pull(True).wait_send())

        def sent_bias():
            bias_pull(False).wait_send()
            bias_relay.wait_send()
        away(sent_bias)
        gather.finish()
        gather.write([full_out], lambda cp: cp.wait())
        for cp in (x_copy, n_copy, b_copy):
            cp.wait()

    shape = (2, 4, n, rows, cols)
    dma = pltpu.SemaphoreType.DMA
    vmem = pl.BlockSpec(memory_space=pltpu.VMEM)
    return pl.pallas_call(
        kernel, in_specs=[ANY, ANY, vmem, vmem, vmem, vmem], out_specs=[ANY] * 4 + [vmem],
        out_shape=[jax.ShapeDtypeStruct(patches.shape, BF), jax.ShapeDtypeStruct(shape, BF),
                   jax.ShapeDtypeStruct((2,) + patches.shape, BF),
                   jax.ShapeDtypeStruct((2,) + small.shape, F32),
                   jax.ShapeDtypeStruct((2, wide, seq), BF)],
        scratch_shapes=[pltpu.VMEM(patches.shape, BF), pltpu.VMEM((2,) + patches.shape, BF),
                        pltpu.VMEM((2,) + small.shape, F32), pltpu.VMEM(shape, BF),
                        dma((Gather.SEMS, n)), dma((Gather.SEMS, n)), dma((4,)),
                        dma((PIECES,)), dma((PIECES,)), dma((PIECES,)), dma((PIECES,)),
                        dma((2,)), dma((2,))],
        compiler_params=pltpu.CompilerParams(collective_id=1, **COMM), name="front",
    )(patches, shard, keep, swap, vectors, small)


def attend(bias, qkv, shards_in, rows_in):
    slots, _, heads, _, seq = qkv.shape
    rows, cols = shards_in[0].shape[2:]
    counts = [v.shape[1] for v in shards_in]
    n = sum(counts)
    block = 512
    parts = seq // block
    steps = slots * heads * parts
    per = 2
    many = len(shards_in)

    def kernel(*refs):
        bias_ref, qkv_ref = refs[:2]
        srcs = refs[2:2 + many]
        x_ref, ctx_ref, lse_ref = refs[2 + many:5 + many]
        outs = refs[5 + many:5 + 2 * many]
        x_out, full, x_buf, send, recv, local, x_send, x_recv, p_send, p_recv = refs[5 + 2 * many:]
        step = pl.program_id(0)
        me = Me()
        gather = Gather(me, srcs, full, send, recv, local)
        cross = Cross(me, x_ref, x_buf.at[0], x_send, x_recv)

        def hand(i):
            return pltpu.make_async_remote_copy(
                src_ref=x_buf.at[0, i], dst_ref=x_buf.at[1, i], send_sem=p_send.at[i],
                recv_sem=p_recv.at[i], device_id=me.core, device_id_type=MESH)

        @pl.when(step == 0)
        def _():
            me.greet()
            gather.keep_own(lambda cp: cp.start())
            gather.prologue()
            gather.keep_own(lambda cp: cp.wait())

        for index in range(per):
            gather.tick(step * per + index)

        @pl.when(step >= steps - PIECES)
        def _():
            cross.start(step - (steps - PIECES))

        k, v = qkv_ref[0, 1, 0], qkv_ref[0, 2, 0]
        at = pl.ds(pl.multiple_of(step % parts * block, block), block)
        q = qkv_ref[0, 0, 0, :, at] * jnp.asarray(HEAD_DIM ** (-0.5), BF)
        scores = dg(jnp.concatenate([k, bias_ref[...]], 0),
                    jnp.concatenate([q, first_row(block)], 0), 0, 0)
        top = jnp.max(scores, 0, keepdims=True)
        powered = jnp.exp(scores - top)
        summed = jnp.concatenate([v, jnp.ones((16, seq), BF)], 0)
        out = dg(summed, powered.astype(BF), 1, 0)
        total = out[HEAD_DIM:HEAD_DIM + 1]
        ctx_ref[0, 0, :, at] = (out[:HEAD_DIM] / total).astype(BF)
        lse_ref[0, 0, :, at] = top + jnp.log(total)

        @pl.when(step == steps - 1)
        def _():
            def rest(index, carry):
                gather.tick(index)
                return carry
            lax.fori_loop(steps * per, max(gather.ticks, steps * per), rest, 0)
            gather.write(outs, lambda cp: cp.start())
            for i in range(PIECES):
                cross.wait(i)
                hand(i).start()
            for i in range(PIECES):
                hand(i).wait_recv()
            x_copy = pltpu.make_async_copy(x_buf, x_out, local.at[many])
            x_copy.start()
            gather.finish()
            cross.drain()
            for i in range(PIECES):
                hand(i).wait_send()
            gather.write(outs, lambda cp: cp.wait())
            x_copy.wait()

    col, tri, one, row = head_specs(heads, seq, parts)
    dma = pltpu.SemaphoreType.DMA
    pairs = slots * heads * seq * seq
    pair = (2,) + rows_in.shape
    return pl.pallas_call(
        kernel, grid=(steps,), in_specs=[col, tri] + [ANY] * (many + 1),
        out_specs=[one, row] + [ANY] * (many + 1),
        out_shape=[jax.ShapeDtypeStruct((slots, heads, HEAD_DIM, seq), BF),
                   jax.ShapeDtypeStruct((slots, heads, 1, seq), F32)]
        + [jax.ShapeDtypeStruct((2, 4, k, rows, cols), BF) for k in counts]
        + [jax.ShapeDtypeStruct(pair, BF)],
        scratch_shapes=[pltpu.VMEM((2, 4, n, rows, cols), BF), pltpu.VMEM(pair, BF),
                        dma((Gather.SEMS, n)), dma((Gather.SEMS, n)), dma((many + 1,)),
                        dma((PIECES,)), dma((PIECES,)), dma((PIECES,)), dma((PIECES,))],
        compiler_params=pltpu.CompilerParams(collective_id=2, **COMM), name="attend",
        cost_estimate=pl.CostEstimate(flops=pairs * 4 * HEAD_DIM, bytes_accessed=qkv.size * 3,
                                      transcendentals=pairs))(bias, qkv, *shards_in, rows_in)


def tail(bias, qkv, do, ctx, lse, g_out, g_up, g_down, rows_out, weights, normed, block_in,
         grad_res, cols_keep, cols_swap, gain, small):
    slots, _, heads, _, seq = qkv.shape
    rows, cols = g_out.shape[3:]
    wide = weights.shape[1]
    counts = [g_out.shape[2], g_up[0].shape[1], g_down[0].shape[1], wide // (4 * rows)]
    n = sum(counts)
    late = n - counts[3]
    block = 256
    parts = seq // block
    steps = slots * heads * parts
    own_rows = seq // 2
    slab = 128
    slabs = own_rows // slab
    hops = 5

    def kernel(bias_ref, qkv_ref, do_ref, ctx_ref, lse_ref, w_ref, n_ref, x_ref, res_ref, keep_ref,
               swap_ref, gain_ref, small_ref, go, gu0, gu1, gd0, gd1, y_ref,
               gp_ref, small_out, fo, fu, fd, fq, y_out, p_out,
               dk_ref, dv_ref, dqkv, gn1, given, taken, sums, incoming, stage, y_buf, p_buf,
               g_send, g_recv, s_send, s_recv, y_send, y_recv, p_send, p_recv, *scratch):
        step = pl.program_id(0)
        me = Me()
        reduce = Reduce(me, scratch)
        cross = Cross(me, y_ref, y_buf, y_send, y_recv)
        home_rows = Cross(me, stage, p_buf, p_send, p_recv)
        t_odd = lax.axis_index("tp") % 2

        def hand(i):
            return pltpu.make_async_remote_copy(
                src_ref=given.at[i], dst_ref=taken.at[i], send_sem=g_send.at[i],
                recv_sem=g_recv.at[i], device_id=me.core, device_id_type=MESH)

        partner = [me.core, me.x, me.y, me.near, me.two]

        def hop(k):
            return pltpu.make_async_remote_copy(
                src_ref=sums.at[k], dst_ref=incoming.at[k], send_sem=s_send.at[k],
                recv_sem=s_recv.at[k], device_id=partner[k], device_id_type=MESH)

        @pl.when(step == 0)
        def _():
            srcs = [go, (gu0, gu1), (gd0, gd1)]
            reduce.load(srcs, lambda cp: cp.start())
            me.greet(two=True)
            reduce.load(srcs, lambda cp: cp.wait())
            reduce.prologue()

        reduce.tick(step)

        @pl.when(step < PIECES)
        def _():
            cross.start(step)

        part = step % parts
        head = step // parts
        slot, at_head = head // heads, head % heads
        at = pl.ds(pl.multiple_of(part * block, block), block)

        def feature(i):
            return pl.ds(pl.multiple_of((i * heads + at_head) * HEAD_DIM, HEAD_DIM), HEAD_DIM)

        k, v = qkv_ref[0, 1, 0], qkv_ref[0, 2, 0]
        q = qkv_ref[0, 0, 0, :, at] * jnp.asarray(HEAD_DIM ** (-0.5), BF)
        dob = do_ref[0, 0, :, at]
        inner = jnp.sum(dob.astype(F32) * ctx_ref[0, 0, :, at].astype(F32), 0, keepdims=True)
        scores = dg(jnp.concatenate([k, bias_ref[...]], 0),
                    jnp.concatenate([q, first_row(block)], 0), 0, 0)
        probs = jnp.exp(scores - lse_ref[0, 0, :, at])
        ds = (probs * (dg(v, dob, 0, 0) - inner)).astype(BF)
        first = part == 0
        dv = dg(dob, probs.astype(BF), 1, 1)
        dk = dg(q, ds, 1, 1)
        dqkv[slot, feature(0), at] = (dg(k, ds, 1, 0) * HEAD_DIM ** (-0.5)).astype(BF)

        @pl.when(first)
        def _():
            dk_ref[...] = dk
            dv_ref[...] = dv

        @pl.when(jnp.logical_not(first))
        def _():
            dk_ref[...] += dk
            dv_ref[...] += dv

        @pl.when(part == parts - 1)
        def _():
            dqkv[slot, feature(1), :] = dk_ref[...].astype(BF)
            dqkv[slot, feature(2), :] = dv_ref[...].astype(BF)

        @pl.when(step == steps - 1)
        def _():
            clock = [steps]

            def tick():
                reduce.tick(jnp.int32(clock[0]))
                clock[0] += 1

            quarter = wide // 4
            for s in range(2):
                def piece(i, carry, s=s):
                    at_rows = pl.ds(pl.multiple_of(i * quarter, 16), quarter)
                    out = dg(dqkv[s, at_rows, :], n_ref[...], 1, 0)
                    reduce.g[s, i, late:] = out.astype(BF).reshape(counts[3], rows, cols)
                    return carry
                lax.fori_loop(0, 4, piece, 0)
                if s == 0:
                    tick()
            sums[0] = small_ref[...]
            ones = jnp.ones((8, seq), BF)
            third = wide // 3
            for s in range(2):
                line = dg(ones, dqkv[s], 1, 1)[0:1]
                line = jnp.concatenate(
                    [line[:, :third], line[:, 2 * third:],
                     jnp.zeros((1, cols - 2 * third), F32)], 1)
                where = 1 + 2 * me.c + (t_odd if s == 0 else 1 - t_odd)
                sums[0, where, 1:2, :] = line

            def partial(low):
                at_rows = pl.ds(pl.multiple_of(low, slab), slab)
                return dg(dqkv[0, :, at_rows], w_ref[0], 0, 0) + dg(dqkv[1, :, at_rows], w_ref[1], 0, 0)

            def other_half(i, carry):
                given[i] = partial(own_rows + i * slab).astype(BF)
                hand(i).start()
                reduce.tick(steps + 1 + i)
                return carry
            lax.fori_loop(0, slabs, other_half, 0)

            def own_half(i, carry):
                gn1[i] = partial(i * slab)
                reduce.tick(steps + 1 + slabs + i)
                return carry
            lax.fori_loop(0, slabs, own_half, 0)

            def norm_back(i, carry):
                d_mask, d_gain, d_bias = carry
                at_rows = pl.ds(pl.multiple_of(i * slab, slab), slab)
                hand(i).wait_recv()
                grad = gn1[i] + taken[i].astype(F32)
                value = x_ref[at_rows, :]
                center = value - jnp.mean(value, -1, keepdims=True)
                scale = lax.rsqrt(jnp.mean(center * center, -1, keepdims=True) + 1e-06)
                unit = center * scale
                turned = grad * gain_ref[0:1, :]
                inside = (turned - jnp.mean(turned, -1, keepdims=True)
                          - unit * jnp.mean(turned * unit, -1, keepdims=True))
                grad_in = res_ref[at_rows, :] + scale * inside
                kept = keep_ref[at_rows, :] * grad_in
                gp_ref[at_rows, :] = kept
                half = slab // 2
                stage[2 * i] = kept[:half].astype(BF)
                stage[2 * i + 1] = kept[half:].astype(BF)
                home_rows.start(2 * i)
                home_rows.start(2 * i + 1)
                reduce.tick(steps + 1 + 2 * slabs + i)
                total = lambda v: jnp.sum(v, 0, keepdims=True)
                return (d_mask + total(swap_ref[at_rows, :] * grad_in),
                        d_gain + total(grad * unit), d_bias + total(grad))
            zero = jnp.zeros((1, cols), F32)
            lines = lax.fori_loop(0, slabs, norm_back, (zero, zero, zero))
            for k in range(3):
                sums[0, 0, k:k + 1, :] = lines[k]
            hop(0).start()
            begin = steps + 1 + 3 * slabs

            def step_on(index, carry):
                reduce.tick(index)
                for k in range(hops):
                    @pl.when(index == begin + 3 * k + 2)
                    def _(k=k):
                        hop(k).wait_recv()
                        sums[k + 1] = sums[k] + incoming[k]
                        if k + 1 < hops:
                            hop(k + 1).start()
                return carry
            lax.fori_loop(begin, max(reduce.ticks, begin + 3 * hops), step_on, 0)
            small_out[...] = sums[hops]
            for i in range(PIECES):
                cross.wait(i)
                home_rows.wait(i)
            y_copy = pltpu.make_async_copy(y_buf, y_out, reduce.local.at[6])
            p_copy = pltpu.make_async_copy(p_buf, p_out, reduce.local.at[7])
            y_copy.start()
            p_copy.start()
            for k in range(hops):
                hop(k).wait_send()
            for i in range(slabs):
                hand(i).wait_send()
            cross.drain()
            home_rows.drain()
            reduce.finish([fo, fu, fd, fq])
            y_copy.wait()
            p_copy.wait()

    col, tri, one, row = head_specs(heads, seq, parts)
    pairs = slots * heads * seq * seq
    dma = pltpu.SemaphoreType.DMA
    vmem = pl.BlockSpec(memory_space=pltpu.VMEM)
    hand_shape = (slabs, slab, cols)
    return pl.pallas_call(
        kernel, grid=(steps,), in_specs=[col, tri, one, one, row] + [vmem] * 8 + [ANY] * 6,
        out_specs=[vmem, vmem] + [ANY] * 6,
        out_shape=[jax.ShapeDtypeStruct((own_rows, cols), F32), jax.ShapeDtypeStruct(small.shape, F32)]
        + [jax.ShapeDtypeStruct((4, k, rows, cols), BF) for k in counts]
        + [jax.ShapeDtypeStruct(rows_out.shape, BF)] * 2,
        scratch_shapes=[pltpu.VMEM((HEAD_DIM, seq), F32)] * 2
        + [pltpu.VMEM((2, wide, seq), BF), pltpu.VMEM(hand_shape, F32), pltpu.VMEM(hand_shape, BF),
           pltpu.VMEM(hand_shape, BF), pltpu.VMEM((hops + 1,) + small.shape, F32),
           pltpu.VMEM((hops,) + small.shape, F32)] + [pltpu.VMEM(rows_out.shape, BF)] * 3
        + [dma((slabs,)), dma((slabs,)), dma((hops,)), dma((hops,))] + Cross.sems() + Cross.sems()
        + Reduce.scratch(n, rows, cols),
        compiler_params=pltpu.CompilerParams(collective_id=3, **COMM), name="tail",
        cost_estimate=pl.CostEstimate(flops=pairs * 10 * HEAD_DIM, bytes_accessed=qkv.size * 6,
                                      transcendentals=pairs),
    )(bias, qkv, do, ctx, lse, weights, normed, block_in, grad_res, cols_keep, cols_swap, gain, small,
      g_out, *g_up, *g_down, rows_out)


def rest(w, total):
    if w.n_dp > 8:
        groups = [[r + 8 * g for g in range(w.n_dp // 8)] for r in range(8)]
        total = lax.psum(total, "dp", axis_index_groups=groups)
    return total


class Wires:
    def __init__(self, n_dp, n_tp):
        assert n_tp == 4 and n_dp % 8 == 0
        self.n_dp, self.n_tp = n_dp, n_tp
        self.core = [(d * n_tp + t, (d ^ 1) * n_tp + t) for d in range(n_dp) for t in range(n_tp)]

    def other(self, value):
        return lax.ppermute(value, AXES, self.core)


def shards(w, patches, validity, mask_pos, mask_token, ln1_gain, ln1_bias, w_qkv, b_qv, w_out,
           b_out, ln2_gain, ln2_bias, w_up, b_up, w_down, b_down, out_grad):
    d, t = lax.axis_index("dp"), lax.axis_index("tp")
    c = d & 1
    rows, width = patches.shape
    seq = validity.shape[1]
    local = w_qkv.shape[2]
    heads = local // HEAD_DIM
    wide = 3 * local
    units = w_up.shape[1]
    both = lambda v: jnp.concatenate([v, w.other(v)], 0)
    swapped = ((d ^ t) & 1) == 1
    pieces = lambda v: v.reshape(PIECES, rows // PIECES, width)
    chunk = lambda v, k: v.reshape(v.shape[:-2] + (4, -1, k, width))

    bucket = t >> 1
    flags = jnp.stack([lax.dynamic_index_in_dim(validity, bucket, 0, False),
                       lax.dynamic_index_in_dim(mask_pos, bucket, 0, False)])
    flags = jnp.where(swapped, w.other(flags), flags)
    own_flags = lax.dynamic_slice_in_dim(flags, c * rows, rows, 1)
    other_flags = lax.dynamic_slice_in_dim(flags, (1 - c) * rows, rows, 1)
    keep_key = jnp.concatenate([own_flags[0], other_flags[0]])
    valid_all = keep_key.astype(F32)[:, None]
    valid_col = valid_all[:rows]
    masked_col = own_flags[1].astype(F32)[:, None]
    keep_token = valid_col * (1.0 - masked_col)
    swap_token = valid_col * masked_col

    vectors = jnp.zeros((8, width), F32).at[0].set(mask_token).at[1].set(ln1_gain).at[2].set(ln1_bias)
    line = jnp.concatenate([b_qv[0], jnp.zeros((local,), F32), b_qv[1],
                            jnp.zeros((width - wide,), F32)])
    small = jnp.zeros((8, width), F32).at[0].set(b_up).at[1].set(line)
    turned = w_qkv.transpose(1, 2, 0).reshape(wide, width)
    patches, wq, normed_all, small, qkv = front(
        pieces(patches), chunk(turned, 16), keep_token, swap_token, vectors, small)
    patches = patches.reshape(rows, width)
    wq = wq.reshape(2, wide, width)
    normed_all = normed_all.reshape(seq, width)
    bias_up = small[:, 0]
    block_in = keep_token * patches.astype(F32) + swap_token * mask_token[None, :]
    slots = (0, 1)
    qkv = qkv.reshape(2, 3, heads, HEAD_DIM, seq)
    key_bias = jnp.zeros((16, seq), BF).at[0].set(
        jnp.where(keep_key > 0, 0.0, -1000000000.0).astype(BF))
    context, log_norm, wo, wu, wd, grad_all = attend(
        key_bias, qkv, [chunk(w_out, CHUNK), chunk(w_up, CHUNK), chunk(w_down, CHUNK)],
        pieces(out_grad))
    wo_rows = wo.reshape(2 * local, width)
    wu = wu.reshape(2, width, units)
    wd = wd.reshape(2, units, width)
    context_rows = context.reshape(2 * local, seq)
    attn_part = outer_sum(context_rows, wo_rows)
    attn_rows = attn_part[:rows] + w.other(attn_part[rows:].astype(BF)).astype(F32)
    residual = block_in + attn_rows + b_out[None, :]
    normed_g, ln2_pull = jax.vjp(layer_norm, residual, ln2_gain, ln2_bias)
    normed_mlp = both(normed_g.astype(BF))
    hidden, gelu_pull = [], []
    for s in slots:
        hidden_pre = dot(normed_mlp, wu[s]) + bias_up[s][None, :]
        gelu_out, pull = jax.vjp(exact_gelu, hidden_pre)
        hidden.append(gelu_out.astype(BF))
        gelu_pull.append(pull)
    mlp_part = dot(hidden[0], wd[0]) + dot(hidden[1], wd[1])
    mlp_rows = mlp_part[:rows] + w.other(mlp_part[rows:].astype(BF)).astype(F32)
    output = (valid_col * (residual + mlp_rows + b_down[None, :])).astype(BF)

    grad_all = (valid_all * grad_all.reshape(seq, width).astype(F32)).astype(BF)
    grad_out = grad_all[:rows].astype(F32)
    grad_b_down = jnp.sum(grad_out, 0)
    g_up, g_down, g_bup, gn2 = [], [], [], 0.0
    for s in slots:
        g_down.append(chunk(outer_sum(hidden[s], grad_all).astype(BF), CHUNK))
        grad_pre = gelu_pull[s](dot_trans(grad_all, wd[s]))[0].astype(BF)
        g_up.append(chunk(outer_sum(normed_mlp, grad_pre).astype(BF), CHUNK))
        g_bup.append(jnp.sum(grad_pre.astype(F32), 0))
        gn2 = gn2 + dot_trans(grad_pre, wu[s])
    gn2 = gn2[:rows] + w.other(gn2[rows:].astype(BF)).astype(F32)
    grad_res_part, grad_ln2_gain, grad_ln2_bias = ln2_pull(gn2)
    grad_res = grad_out + grad_res_part
    grad_b_out = jnp.sum(grad_res, 0)
    grad_res_all = both(grad_res.astype(BF))
    g_out = chunk(dot(context_rows, grad_res_all).astype(BF).reshape(2, local, width), CHUNK)
    grad_context = dot_trans(wo_rows, grad_res_all).astype(BF)
    empty = jnp.zeros((3, width), F32)
    shared = jnp.concatenate([empty, jnp.stack([grad_b_out, grad_ln2_gain, grad_ln2_bias,
                                                grad_b_down]), empty[:1]])
    pair = jnp.stack(g_bup)
    pair = jnp.where((t & 1) == 0, pair, pair[::-1])
    quads = jnp.where(c == 0, jnp.concatenate([pair, jnp.zeros_like(pair)]),
                      jnp.concatenate([jnp.zeros_like(pair), pair]))
    quads = jnp.pad(quads[:, None], ((0, 0), (0, 7), (0, 0)))
    grad_patches, totals, f_out, f_up, f_down, f_qkv, output, moved = tail(
        key_bias, qkv, grad_context.reshape(context.shape), context, log_norm, g_out, g_up, g_down,
        pieces(output), wq, normed_all, block_in, grad_res, keep_token, swap_token, vectors[1:2],
        jnp.concatenate([shared[None], quads]))
    output = output.reshape(rows, width)
    grad_patches = jnp.where(swapped, moved.reshape(rows, width).astype(F32), grad_patches)
    totals = rest(w, totals)
    mine = lax.dynamic_index_in_dim(totals, 1 + t, 0, False)
    totals = totals[0]
    whole = lambda v: rest(w, v.reshape(-1, width).astype(F32))
    grad_w_qkv = whole(f_qkv).reshape(3, local, width).transpose(2, 0, 1)
    return (output, grad_patches, totals[0], totals[1], totals[2], grad_w_qkv,
            mine[1, :2 * local].reshape(2, local), whole(f_out), totals[3], totals[4], totals[5],
            whole(f_up), mine[0], whole(f_down), totals[6])


def solution(mesh):
    w = Wires(mesh.shape["dp"], mesh.shape["tp"])
    rows, cols = P(AXES, None), P(None, "tp")
    return jax.shard_map(
        lambda *args: shards(w, *args),
        mesh=mesh,
        in_specs=(rows, P("dp", None), P("dp", None), P(), P(), P(), P(None, None, "tp"), cols,
                  P("tp", None), P(), P(), P(), cols, P("tp"), P("tp", None), P(), rows),
        out_specs=(rows, rows, P(), P(), P(), P(None, None, "tp"), cols, P("tp", None), P(), P(),
                   P(), cols, P("tp"), P("tp", None), P()),
        check_vma=False,
    )
```

```python
import jax
import jax.numpy as jnp
from jax import lax
from jax.experimental import pallas as pl
from jax.experimental.pallas import tpu as pltpu
from jax.sharding import PartitionSpec as P

HEAD_DIM = 64
GAP = 4
PIECES = 4
CHUNK = 16
AXES = ("dp", "tp")
BF = jnp.bfloat16
F32 = jnp.float32


def dg(left, right, ldim, rdim):
    return lax.dot_general(left, right, (((ldim,), (rdim,)), ((), ())), preferred_element_type=F32)


def first_row(block):
    return jnp.where(lax.broadcasted_iota(jnp.int32, (16, block), 0) < 1, 1.0, 0.0).astype(BF)


def head_specs(heads, seq, parts):
    head = lambda i: (i // parts // heads, i // parts % heads)
    col = pl.BlockSpec((16, seq), lambda i: (0, 0))
    tri = pl.BlockSpec((1, 3, 1, HEAD_DIM, seq), lambda i: (head(i)[0], 0, head(i)[1], 0, 0))
    one = pl.BlockSpec((1, 1, HEAD_DIM, seq), lambda i: head(i) + (0, 0))
    row = pl.BlockSpec((1, 1, 1, seq), lambda i: head(i) + (0, 0))
    return col, tri, one, row


class Me:
    def __init__(self):
        d, t = lax.axis_index("dp"), lax.axis_index("tp")
        c, qx, qy = d % 2, (d // 2) % 2, (d // 4) % 2
        self.c = c
        self.home = (t // 2 + c + 1) % 2
        self.swapped = (d + t) % 2
        self.core = {"dp": d + 1 - 2 * c, "tp": t}
        self.x = {"dp": d + 2 - 4 * qx, "tp": t}
        self.y = {"dp": d + 4 - 8 * qy, "tp": t}
        self.near = {"dp": d, "tp": t + 1 - 2 * (t % 2)}
        self.far = {"dp": d + 1 - 2 * c, "tp": 2 * c + t % 2}
        self.cross = {"dp": d + 1 - 2 * c, "tp": t + 1 - 2 * (t % 2)}
        self.two = {"dp": d, "tp": t + 2 - 4 * (t // 2)}
        self.q = [qx + 2 * qy, 1 - qx + 2 * qy, qx + 2 * (1 - qy), 1 - qx + 2 * (1 - qy)]

    def greet(self, swap=True, two=False):
        barrier = pltpu.get_barrier_semaphore()
        others = [self.core, self.x, self.y, self.near] + ([self.two] if two else [])
        for other in others:
            pl.semaphore_signal(barrier, inc=1, device_id=other, device_id_type=MESH)

        @pl.when(self.home == 0)
        def _():
            pl.semaphore_signal(barrier, inc=1, device_id=self.far, device_id_type=MESH)

        if swap:
            @pl.when(self.swapped == 1)
            def _():
                pl.semaphore_signal(barrier, inc=1, device_id=self.cross, device_id_type=MESH)

        extra = self.swapped if swap else 0
        pl.semaphore_wait(barrier, len(others) + 1 - self.home + extra)


class Cross:
    @staticmethod
    def sems():
        return [pltpu.SemaphoreType.DMA((PIECES,)), pltpu.SemaphoreType.DMA((PIECES,))]

    def __init__(self, me, src, dst, send, recv):
        self.me, self.src, self.dst, self.send, self.recv = me, src, dst, send, recv

    def copy(self, i):
        return pltpu.make_async_remote_copy(
            src_ref=self.src.at[i], dst_ref=self.dst.at[i], send_sem=self.send.at[i],
            recv_sem=self.recv.at[i], device_id=self.me.cross, device_id_type=MESH)

    def keep(self, i):
        return pltpu.make_async_copy(self.src.at[i], self.dst.at[i], self.recv.at[i])

    def start(self, i):
        @pl.when(self.me.swapped == 1)
        def _():
            self.copy(i).start()

        @pl.when(self.me.swapped == 0)
        def _():
            self.keep(i).start()

    def wait(self, i):
        @pl.when(self.me.swapped == 1)
        def _():
            self.copy(i).wait_recv()

        @pl.when(self.me.swapped == 0)
        def _():
            self.keep(i).wait()

    def drain(self):
        @pl.when(self.me.swapped == 1)
        def _():
            for i in range(PIECES):
                self.copy(i).wait_send()


class Gather:
    STAGES = 4
    SEMS = 6

    def __init__(self, me, srcs, full, send, recv, local):
        self.me, self.srcs, self.full, self.send, self.recv = me, srcs, full, send, recv
        self.local = local
        self.n = full.shape[2]
        self.spans = spans(srcs)

    def keep_own(self, act):
        @pl.when(self.me.home == 1)
        def _():
            for i, (src, (low, high)) in enumerate(zip(self.srcs, self.spans)):
                act(pltpu.make_async_copy(src, self.full.at[0, :, pl.ds(low, high - low)],
                                          self.local.at[i]))

    def copy(self, kind, n, src, dst, device):
        return pltpu.make_async_remote_copy(
            src_ref=src, dst_ref=dst, send_sem=self.send.at[kind, n],
            recv_sem=self.recv.at[kind, n], device_id=device, device_id_type=MESH)

    def pull(self, n, home, src=None):
        me, q = self.me, self.me.q[0]
        slot = 1 if home else 0
        src = self.full.at[slot, q, n] if src is None else src
        return self.copy(0, n, src, self.full.at[slot, q, n], me.near if home else me.far)

    def relay(self, n):
        q = self.me.q[0]
        return self.copy(1, n, self.full.at[0, q, n], self.full.at[1, q, n], self.me.near)

    def plane(self, n, home):
        q, first = self.me.q[0], (1 if home else 0)
        part = self.full.at[pl.ds(first, 2 - first), q, n]
        return [self.copy(2, n, part, part, self.me.x), self.copy(3, n, part, part, self.me.y)]

    def diag(self, n, slot, through_x):
        if through_x:
            part = self.full.at[slot, self.me.q[2], n]
            return self.copy(4, n, part, part, self.me.x)
        part = self.full.at[slot, self.me.q[1], n]
        return self.copy(5, n, part, part, self.me.y)

    def diags(self, n, home, act):
        if home:
            @pl.when(n % 2 == 0)
            def _():
                act(self.diag(n, 1, True))

            @pl.when(n % 2 == 1)
            def _():
                act(self.diag(n, 1, False))
        else:
            act(self.diag(n, 0, True))
            act(self.diag(n, 1, False))

    def sides(self, body):
        @pl.when(self.me.home == 1)
        def _():
            body(True)

        @pl.when(self.me.home == 0)
        def _():
            body(False)

    def start(self, n):
        @pl.when(n < self.n)
        def _():
            for src, (low, high) in zip(self.srcs, self.spans):
                @pl.when(jnp.logical_and(n >= low, n < high))
                def _(src=src, low=low):
                    part = src.at[self.me.q[0], n - low]
                    self.sides(lambda home: self.pull(n, home, part).start())

    def prologue(self):
        self.start(jnp.int32(0))
        self.start(jnp.int32(1))

    def tick(self, step):
        def stage(n, body):
            @pl.when(jnp.logical_and(n >= 0, n < self.n))
            def _():
                body(n)

        def four(n):
            self.sides(lambda home: self.diags(n, home, lambda c: c.wait_recv()))

        def three(n):
            def side(home):
                for c in self.plane(n, home):
                    c.wait_recv()
                self.diags(n, home, lambda c: c.start())
            self.sides(side)

        def two(n):
            def side(home):
                if not home:
                    self.relay(n).wait_recv()
                for c in self.plane(n, home):
                    c.start()
            self.sides(side)

        def one(n):
            def side(home):
                self.pull(n, home).wait_recv()
                if not home:
                    self.relay(n).start()
            self.sides(side)

        for index, body in reversed(list(enumerate([one, two, three, four]))):
            stage(step - 1 - GAP * index, body)
        self.start(step + 2)

    @property
    def ticks(self):
        return self.n + 1 + GAP * (self.STAGES - 1)

    def finish(self):
        def drain(n, carry):
            def side(home):
                self.pull(n, home).wait_send()
                if not home:
                    self.relay(n).wait_send()
                for c in self.plane(n, home):
                    c.wait_send()
                self.diags(n, home, lambda c: c.wait_send())
            self.sides(side)
            return carry
        lax.fori_loop(0, self.n, drain, 0)

    def write(self, outs, act):
        for i, (out, (low, high)) in enumerate(zip(outs, self.spans)):
            act(pltpu.make_async_copy(self.full.at[:, :, pl.ds(low, high - low)], out,
                                      self.local.at[i]))


class Reduce:
    STAGES = 8
    SEMS = 11

    @staticmethod
    def scratch(n, rows, cols):
        piece = (rows, cols)
        return [
            pltpu.VMEM((2, 4, n) + piece, BF), pltpu.VMEM((n,) + piece, BF),
            pltpu.VMEM((n,) + piece, BF), pltpu.VMEM((2, n) + piece, BF),
            pltpu.VMEM((2, n) + piece, BF), pltpu.VMEM((n,) + piece, BF),
            pltpu.VMEM((n,) + piece, BF), pltpu.VMEM((n,) + piece, BF),
            pltpu.VMEM((n,) + piece, BF), pltpu.VMEM((n,) + piece, F32),
            pltpu.VMEM((4, n) + piece, BF),
            pltpu.SemaphoreType.DMA((Reduce.SEMS, n)), pltpu.SemaphoreType.DMA((Reduce.SEMS, n)),
            pltpu.SemaphoreType.DMA((8,)),
        ]

    def __init__(self, me, refs):
        (self.g, self.ax, self.by, self.tx, self.ty, self.back, self.got, self.give, self.take,
         self.acc, self.fin, self.send, self.recv, self.local) = refs
        self.me = me
        self.n = self.g.shape[2]

    def copy(self, kind, n, src, dst, device):
        return pltpu.make_async_remote_copy(
            src_ref=src, dst_ref=dst, send_sem=self.send.at[kind, n],
            recv_sem=self.recv.at[kind, n], device_id=device, device_id_type=MESH)

    def corner(self, n):
        q = self.me.q[3]
        return [self.copy(0, n, self.g.at[0, q, n], self.ax.at[n], self.me.x),
                self.copy(1, n, self.g.at[1, q, n], self.by.at[n], self.me.y)]

    def side(self, n):
        q = self.me.q
        return [self.copy(2, n, self.g.at[:, q[1], n], self.tx.at[:, n], self.me.x),
                self.copy(3, n, self.g.at[:, q[2], n], self.ty.at[:, n], self.me.y)]

    def second(self, n):
        return self.copy(4, n, self.g.at[1, self.me.q[0], n], self.back.at[n], self.me.near)

    def push(self, n, home):
        q = self.me.q[0]
        if home:
            return self.copy(5, n, self.g.at[1, q, n], self.got.at[n], self.me.near)
        return self.copy(5, n, self.g.at[0, q, n], self.got.at[n], self.me.far)

    def pair(self, n):
        return self.copy(6, n, self.give.at[n], self.take.at[n], self.me.core)

    def spread(self, n):
        part = self.fin.at[self.me.q[0], n]
        return [self.copy(7, n, part, part, self.me.x), self.copy(8, n, part, part, self.me.y)]

    def diag(self, n, act):
        @pl.when(n // 2 % 2 == 0)
        def _():
            part = self.fin.at[self.me.q[2], n]
            act(self.copy(9, n, part, part, self.me.x))

        @pl.when(n // 2 % 2 == 1)
        def _():
            part = self.fin.at[self.me.q[1], n]
            act(self.copy(9, n, part, part, self.me.y))

    def share(self, n):
        part = self.fin.at[:, n]
        return self.copy(10, n, part, part, self.me.core)

    def owner(self, n, body):
        pl.when((n + self.me.c) % 2 == 0)(body)

    def helper(self, n, body):
        pl.when((n + self.me.c) % 2 == 1)(body)

    def start(self, n):
        @pl.when(n < self.n)
        def _():
            for c in self.corner(n):
                c.start()

    def load(self, srcs, act):
        index, low = 0, 0
        for src in srcs:
            pair = isinstance(src, tuple)
            count = (src[0] if pair else src).shape[1 if pair else 2]
            for slot in ((0, 1) if pair else (None,)):
                part = self.g.at[slot if pair else slice(None), :, pl.ds(low, count)]
                act(pltpu.make_async_copy(src[slot] if pair else src, part, self.local.at[index]))
                index += 1
            low += count

    def prologue(self):
        self.start(jnp.int32(0))
        self.start(jnp.int32(1))

    def tick(self, step):
        me, g, acc = self.me, self.g, self.acc
        q, c = me.q, me.c
        home_f = me.home.astype(F32)

        def stage(n, body):
            @pl.when(jnp.logical_and(n >= 0, n < self.n))
            def _():
                body(n)

        def away(body):
            pl.when(me.home == 0)(body)

        def at_home(body):
            pl.when(me.home == 1)(body)

        def eight(n):
            self.helper(n, lambda: self.share(n).wait_recv())

        def seven(n):
            def own():
                self.diag(n, lambda cp: cp.wait_recv())
                self.share(n).start()
            self.owner(n, own)

        def six(n):
            def own():
                for cp in self.spread(n):
                    cp.wait_recv()
                self.diag(n, lambda cp: cp.start())
            self.owner(n, own)

        def five(n):
            def own():
                self.pair(n).wait_recv()
                self.fin[q[0], n] = (acc[n] + self.take[n].astype(F32)).astype(BF)
                for cp in self.spread(n):
                    cp.start()
            self.owner(n, own)

        def four(n):
            at_home(lambda: self.push(n, True).wait_recv())
            away(lambda: self.push(n, False).wait_recv())
            total = acc[n] * home_f + self.got[n].astype(F32)

            def own():
                acc[n] = total

            def help_out():
                self.give[n] = total.astype(BF)
                self.pair(n).start()
            self.owner(n, own)
            self.helper(n, help_out)

        def three(n):
            def side():
                self.second(n).wait_recv()
                g[0, q[0], n] = (acc[n] + self.back[n].astype(F32)).astype(BF)
                self.push(n, False).start()
            away(side)

        def two(n):
            for cp in self.side(n):
                cp.wait_recv()
            g[1, q[0], n] = (g[1, q[0], n].astype(F32) + self.tx[1, n].astype(F32)
                             + self.ty[1, n].astype(F32)).astype(BF)
            away(lambda: self.second(n).start())
            at_home(lambda: self.push(n, True).start())
            acc[n] = (g[0, q[0], n].astype(F32) + self.tx[0, n].astype(F32)
                      + self.ty[0, n].astype(F32))

        def one(n):
            for cp in self.corner(n):
                cp.wait_recv()
            g[1, q[1], n] = (g[1, q[1], n].astype(F32) + self.by[n].astype(F32)).astype(BF)
            g[0, q[2], n] = (g[0, q[2], n].astype(F32) + self.ax[n].astype(F32)).astype(BF)
            for cp in self.side(n):
                cp.start()

        bodies = [one, two, three, four, five, six, seven, eight]
        for index in reversed(range(8)):
            stage(step - 1 - GAP * index, bodies[index])
        self.start(step + 2)

    @property
    def ticks(self):
        return self.n + 1 + GAP * (self.STAGES - 1)

    def finish(self, outs):
        def drain(n, carry):
            for cp in self.corner(n) + self.side(n):
                cp.wait_send()

            @pl.when(self.me.home == 1)
            def _():
                self.push(n, True).wait_send()

            @pl.when(self.me.home == 0)
            def _():
                self.second(n).wait_send()
                self.push(n, False).wait_send()

            def own():
                for cp in self.spread(n) + [self.share(n)]:
                    cp.wait_send()
                self.diag(n, lambda cp: cp.wait_send())
            self.owner(n, own)
            self.helper(n, lambda: self.pair(n).wait_send())
            return carry
        lax.fori_loop(0, self.n, drain, 0)
        copies, low = [], 0
        for i, out in enumerate(outs):
            count = out.shape[1]
            copies.append(pltpu.make_async_copy(self.fin.at[:, pl.ds(low, count)], out,
                                                self.local.at[i]))
            low += count
        for cp in copies:
            cp.start()
        for cp in copies:
            cp.wait()


def spans(srcs):
    result, low = [], 0
    for src in srcs:
        result.append((low, low + src.shape[1]))
        low += src.shape[1]
    return result


MESH = pl.DeviceIdType.MESH
COMM = dict(has_side_effects=True, vmem_limit_bytes=60 * 1024 * 1024)
ANY = pl.BlockSpec(memory_space=pl.ANY)


def stats(value):
    center = value - jnp.mean(value, -1, keepdims=True)
    scale = lax.rsqrt(jnp.mean(center * center, -1, keepdims=True) + 1e-06)
    return center, scale


def flag_rows(flags_ref, at, which, cols):
    pick = jnp.where(lax.broadcasted_iota(jnp.int32, (16, cols), 0) == which, 1.0, 0.0)
    return dg(flags_ref[:, at], pick.astype(BF), 0, 0)


def total_rows(value):
    return jnp.sum(value, 0, keepdims=True)


def forward(patches, out_grad, shards_in, flags, bias, vectors, small):
    rows, cols = shards_in[0].shape[2:]
    counts = [v.shape[1] for v in shards_in]
    n = sum(counts)
    piece = patches.shape[1]
    own = PIECES * piece
    seq = 2 * own
    slab = 128
    slabs = own // slab
    wide = 4 * rows * counts[0]
    local = 4 * rows * counts[1]
    units = 4 * rows * counts[3]
    third = wide // 3
    heads = local // HEAD_DIM
    low = [sum(counts[:i]) for i in range(5)]
    block = 512
    parts = seq // block
    wave = 256
    waves = seq // wave

    def kernel(x_ref, y_ref, s0, s1, s2, s3, flags_ref, bias_ref, vec_ref, small_ref,
               wq_out, normed_out, qkv_ref, ctx_ref, lse_ref, do_ref, block_ref, res_ref, out_ref,
               sums_ref, go_ref, gu_out, gd_out,
               x_buf, y_buf, normed, small_buf, full, second, own_f, given, taken, residual, hidden,
               grad_pre, mlp_own, gn2_own, m_give, m_take, gres, gu, gd,
               send, recv, local_sem, x_send, x_recv, y_send, y_recv, hand_send, hand_recv):
        me = Me()
        srcs = [s0, s1, s2, s3]
        gather = Gather(me, srcs, full, send, recv, local_sem)
        cross_x = Cross(me, x_ref, x_buf, x_send, x_recv)
        cross_y = Cross(me, y_ref, y_buf.at[pl.ds(0, PIECES)], y_send, y_recv)

        def hand(kind, i, src, dst):
            return pltpu.make_async_remote_copy(
                src_ref=src, dst_ref=dst, send_sem=hand_send.at[kind, i],
                recv_sem=hand_recv.at[kind, i], device_id=me.core, device_id_type=MESH)

        def hand_n1(i):
            return hand(0, i, normed.at[0, i], normed.at[1, i])

        def hand_y(i):
            return hand(1, i, y_buf.at[i], y_buf.at[PIECES + i])

        def hand_attn(i):
            return hand(2, i, given.at[i], taken.at[i])

        def hand_n2(i):
            return hand(3, i, second.at[i], second.at[slabs + i])

        def hand_mlp(i):
            return hand(4, i, m_give.at[0, i], m_take.at[0, i])

        def hand_gn2(i):
            return hand(5, i, m_give.at[1, i], m_take.at[1, i])

        def hand_res(i):
            return hand(6, i, gres.at[i], gres.at[slabs + i])

        def bias_pull(at_home):
            return pltpu.make_async_remote_copy(
                src_ref=small_ref, dst_ref=small_buf.at[1 if at_home else 0],
                send_sem=hand_send.at[7, 0], recv_sem=hand_recv.at[7, 0],
                device_id=me.near if at_home else me.far, device_id_type=MESH)

        bias_relay = pltpu.make_async_remote_copy(
            src_ref=small_buf.at[0], dst_ref=small_buf.at[1], send_sem=hand_send.at[7, 1],
            recv_sem=hand_recv.at[7, 1], device_id=me.near, device_id_type=MESH)
        bias_keep = pltpu.make_async_copy(small_ref, small_buf.at[0], local_sem.at[4])

        def home(body):
            pl.when(me.home == 1)(body)

        def away(body):
            pl.when(me.home == 0)(body)

        def at_slab(i, size=slab):
            return pl.ds(pl.multiple_of(i * size, size), size)

        def weight(slot, which):
            part = full[slot, :, low[which]:low[which + 1]]
            return part.reshape(4 * rows * counts[which], cols)

        me.greet()
        gather.keep_own(lambda cp: cp.start())
        home(lambda: bias_keep.start())
        home(lambda: bias_pull(True).start())
        away(lambda: bias_pull(False).start())
        gather.prologue()
        cross_x.start(0)
        cross_x.start(1)
        gather.keep_own(lambda cp: cp.wait())

        def first_norm(i):
            at = at_slab(i, piece)
            valid = flag_rows(flags_ref, at, 0, cols)
            masked = flag_rows(flags_ref, at, 1, cols)
            value = (valid * (1.0 - masked) * x_buf[i].astype(F32)
                     + valid * masked * vec_ref[0:1, :])
            block_ref[at, :] = value
            center, scale = stats(value)
            normed[0, i] = (center * scale * vec_ref[1:2, :] + vec_ref[2:3, :]).astype(BF)

        def step(index, carry):
            gather.tick(index)

            @pl.when(index < PIECES - 2)
            def _():
                cross_x.start(index + 2)

            @pl.when(jnp.logical_and(index >= 1, index < PIECES + 1))
            def _():
                cross_x.wait(index - 1)
                first_norm(index - 1)
                hand_n1(index - 1).start()

            @pl.when(index == 4)
            def _():
                def relay():
                    bias_pull(False).wait_recv()
                    bias_relay.start()
                away(relay)
            return carry
        clock = max(counts[0] + 1 + 3 * GAP, PIECES + 1)
        lax.fori_loop(0, clock, step, 0)
        for i in range(PIECES):
            hand_n1(i).wait_recv()

        def own_bias():
            bias_keep.wait()
            bias_pull(True).wait_recv()
        home(own_bias)
        away(lambda: bias_relay.wait_recv())
        rows_all = normed[...].reshape(seq, cols)
        ones = jnp.where(lax.broadcasted_iota(jnp.int32, (16, seq), 0) < 2, 1.0, 0.0).astype(BF)
        for slot in range(2):
            line = small_buf[slot, 1:2, :]
            high = line.astype(BF)
            rest_of = (line - high.astype(F32)).astype(BF)
            pair = jnp.concatenate([high, rest_of, jnp.zeros((14, cols), BF)], 0)[:, :wide]
            weights = weight(slot, 0)
            for part in range(3):
                at = slice(part * third, part * third + third)
                out = dg(weights[at], rows_all, 1, 1) + dg(pair[:, at], ones, 0, 0)
                qkv_ref[slot, at] = out.astype(BF)
        wq_copy = pltpu.make_async_copy(full.at[:, :, pl.ds(0, counts[0])], wq_out, local_sem.at[5])
        n_copy = pltpu.make_async_copy(normed, normed_out, local_sem.at[6])
        wq_copy.start()
        n_copy.start()

        def attention(index, carry):
            gather.tick(clock + index)

            @pl.when(index >= 2 * heads * parts - PIECES)
            def _():
                cross_y.start(index - (2 * heads * parts - PIECES))

            head = index // parts
            slot, at_head = head // heads, head % heads

            def feature(i):
                return pl.ds(pl.multiple_of((i * heads + at_head) * HEAD_DIM, HEAD_DIM), HEAD_DIM)

            at = at_slab(index % parts, block)
            k, v = qkv_ref[slot, feature(1), :], qkv_ref[slot, feature(2), :]
            q = qkv_ref[slot, feature(0), at] * jnp.asarray(HEAD_DIM ** (-0.5), BF)
            scores = dg(jnp.concatenate([k, bias_ref[...]], 0),
                        jnp.concatenate([q, first_row(block)], 0), 0, 0)
            top = jnp.max(scores, 0, keepdims=True)
            powered = jnp.exp(scores - top)
            summed = jnp.concatenate([v, jnp.ones((16, seq), BF)], 0)
            out = dg(summed, powered.astype(BF), 1, 0)
            total = out[HEAD_DIM:HEAD_DIM + 1]
            ctx_ref[pl.ds(pl.multiple_of(head * HEAD_DIM, HEAD_DIM), HEAD_DIM), at] = (
                out[:HEAD_DIM] / total).astype(BF)
            lse_ref[head, :, at] = top + jnp.log(total)
            return carry
        lax.fori_loop(0, 2 * heads * parts, attention, 0)
        clock = clock + 2 * heads * parts

        def projected(i):
            at = at_slab(i)
            return (dg(ctx_ref[0:local, at], weight(0, 1), 0, 0)
                    + dg(ctx_ref[local:2 * local, at], weight(1, 1), 0, 0))

        def other_half(i, carry):
            given[i] = projected(slabs + i).astype(BF)
            hand_attn(i).start()
            gather.tick(clock + i)
            return carry
        lax.fori_loop(0, slabs, other_half, 0)

        def own_half(i, carry):
            own_f[i] = projected(i)
            gather.tick(clock + slabs + i)
            return carry
        lax.fori_loop(0, slabs, own_half, 0)

        def second_norm(i, carry):
            hand_attn(i).wait_recv()
            value = (block_ref[at_slab(i), :] + own_f[i] + taken[i].astype(F32)
                     + vec_ref[3:4, :])
            residual[i] = value
            center, scale = stats(value)
            second[i] = (center * scale * vec_ref[4:5, :] + vec_ref[5:6, :]).astype(BF)
            hand_n2(i).start()
            gather.tick(clock + 2 * slabs + i)
            return carry
        lax.fori_loop(0, slabs, second_norm, 0)
        clock = clock + 3 * slabs

        def more(index, carry):
            gather.tick(index)
            return carry
        lax.fori_loop(clock, max(gather.ticks, clock), more, 0)

        def mask_rows(i, carry):
            cross_y.wait(i)
            g = flag_rows(flags_ref, at_slab(i, piece), 0, cols) * y_buf[i].astype(F32)
            y_buf[i] = g.astype(BF)
            hand_y(i).start()
            return carry + total_rows(g)
        zero = jnp.zeros((1, cols), F32)
        d_b_down = lax.fori_loop(0, PIECES, mask_rows, zero)
        for i in range(slabs):
            hand_n2(i).wait_recv()
        for i in range(PIECES):
            hand_y(i).wait_recv()

        def mlp(b, carry):
            at = at_slab(b, wave)
            n2 = second[pl.ds(b * (wave // slab), wave // slab)].reshape(wave, cols)
            g = y_buf[pl.ds(b * (wave // piece), wave // piece)].reshape(wave, cols)
            forward_sum, backward_sum, lines = 0.0, 0.0, []
            for slot in range(2):
                up, down = weight(slot, 2), weight(slot, 3)
                pre = dg(n2, up, 1, 0) + small_buf[slot, 0:1, :]
                cdf = 0.5 * (1.0 + lax.erf(pre * (0.5 ** 0.5)))
                pdf = jnp.exp(-0.5 * pre * pre) * 0.3989422804014327
                act = (pre * cdf).astype(BF)
                grad = (dg(g, down, 1, 1) * (cdf + pre * pdf)).astype(BF)
                hidden[slot, at, :] = act
                grad_pre[slot, at, :] = grad
                lines.append(carry[slot] + total_rows(grad.astype(F32)))
                forward_sum = forward_sum + dg(act, down, 1, 0)
                backward_sum = backward_sum + dg(grad, up, 1, 1)

            @pl.when(b < waves // 2)
            def _():
                mlp_own[at, :] = forward_sum
                gn2_own[at, :] = backward_sum

            @pl.when(b >= waves // 2)
            def _():
                i = b - waves // 2
                m_give[0, i] = forward_sum.astype(BF)
                m_give[1, i] = backward_sum.astype(BF)
                hand_mlp(i).start()
                hand_gn2(i).start()
            return tuple(lines)
        d_b_up = lax.fori_loop(0, waves, mlp, (zero, zero))

        n2_all = second[...].reshape(seq, cols)
        g_all = y_buf[...].reshape(seq, cols)
        per = 256 // rows
        for slot in range(2):
            for j in range(units // 256):
                at = slice(j * 256, j * 256 + 256)
                out = dg(hidden[slot, :, at], g_all, 0, 0)
                gd[slot, j * per:(j + 1) * per] = out.astype(BF).reshape(per, rows, cols)
        gd_copy = pltpu.make_async_copy(gd, gd_out, local_sem.at[7])
        gd_copy.start()
        for slot in range(2):
            for j in range(cols // 256):
                at = slice(j * 256, j * 256 + 256)
                out = dg(n2_all[:, at], grad_pre[slot], 0, 0)
                gu[slot, j * per:(j + 1) * per] = out.astype(BF).reshape(per, rows, cols)
        gu_copy = pltpu.make_async_copy(gu, gu_out, local_sem.at[8])
        gu_copy.start()
        for i in range(waves // 2):
            hand_gn2(i).wait_recv()

        def second_back(i, carry):
            d_gain, d_bias, d_out = carry
            at = at_slab(i)
            grad = gn2_own[at, :] + m_take[1, i // (wave // slab), at_slab(i % (wave // slab)), :].astype(F32)
            center, scale = stats(residual[i])
            unit = center * scale
            turned = grad * vec_ref[4:5, :]
            inside = (turned - jnp.mean(turned, -1, keepdims=True)
                      - unit * jnp.mean(turned * unit, -1, keepdims=True))
            g = y_buf[pl.ds(i * (slab // piece), slab // piece)].reshape(slab, cols).astype(F32)
            value = g + scale * inside
            res_ref[at, :] = value
            gres[i] = value.astype(BF)
            hand_res(i).start()
            return (d_gain + total_rows(grad * unit), d_bias + total_rows(grad),
                    d_out + total_rows(value))
        d_gain, d_bias, d_out = lax.fori_loop(0, slabs, second_back, (zero, zero, zero))
        for i in range(waves // 2):
            hand_mlp(i).wait_recv()

        def result(i, carry):
            at = at_slab(i)
            value = (residual[i] + mlp_own[at, :] + vec_ref[6:7, :]
                     + m_take[0, i // (wave // slab), at_slab(i % (wave // slab)), :].astype(F32))
            out = flag_rows(flags_ref, at, 0, cols) * value
            out_ref[pl.ds(i * (slab // piece), slab // piece)] = (
                out.astype(BF).reshape(slab // piece, piece, cols))
            return carry
        lax.fori_loop(0, slabs, result, 0)
        sums_ref[...] = jnp.zeros(sums_ref.shape, F32)
        for k, line in enumerate((d_out, d_gain, d_bias, d_b_down)):
            sums_ref[0, 3 + k:4 + k, :] = line
        t_odd = lax.axis_index("tp") % 2
        for slot in range(2):
            sums_ref[1 + 2 * me.c + (t_odd if slot == 0 else 1 - t_odd), 0:1, :] = d_b_up[slot]
        for i in range(slabs):
            hand_res(i).wait_recv()
        res_all = gres[...].reshape(seq, cols)
        for slot in range(2):
            at = slice(slot * local, slot * local + local)
            do_ref[at, :] = dg(weight(slot, 1), res_all, 1, 1).astype(BF)
            out = dg(ctx_ref[at, :], res_all, 1, 0)
            go_ref[slot] = out.astype(BF).reshape(local // rows, rows, cols)
        for i in range(PIECES):
            hand_n1(i).wait_send()
            hand_y(i).wait_send()
        for i in range(slabs):
            hand_attn(i).wait_send()
            hand_n2(i).wait_send()
            hand_res(i).wait_send()
        for i in range(waves // 2):
            hand_mlp(i).wait_send()
            hand_gn2(i).wait_send()
        cross_x.drain()
        cross_y.drain()
        home(lambda: bias_pull(True).wait_send())

        def sent_bias():
            bias_pull(False).wait_send()
            bias_relay.wait_send()
        away(sent_bias)
        gather.finish()
        for cp in (wq_copy, n_copy, gd_copy, gu_copy):
            cp.wait()

    dma = pltpu.SemaphoreType.DMA
    vmem = pl.BlockSpec(memory_space=pltpu.VMEM)
    shape = jax.ShapeDtypeStruct
    slab_shape = (slabs, slab, cols)
    return pl.pallas_call(
        kernel, in_specs=[ANY] * 6 + [vmem] * 4,
        out_specs=[ANY, ANY] + [vmem] * 9 + [ANY, ANY],
        out_shape=[shape((2, 4, counts[0], rows, cols), BF), shape((2,) + patches.shape, BF),
                   shape((2, wide, seq), BF), shape((2 * local, seq), BF),
                   shape((2 * heads, 1, seq), F32), shape((2 * local, seq), BF),
                   shape((own, cols), F32), shape((own, cols), F32), shape(patches.shape, BF),
                   shape((5, 8, cols), F32), shape((2, local // rows, rows, cols), BF),
                   shape((2, cols // rows, rows, cols), BF), shape((2, units // rows, rows, cols), BF)],
        scratch_shapes=[
            pltpu.VMEM(patches.shape, BF), pltpu.VMEM((2 * PIECES,) + patches.shape[1:], BF),
            pltpu.VMEM((2,) + patches.shape, BF), pltpu.VMEM((2,) + small.shape, F32),
            pltpu.VMEM((2, 4, n, rows, cols), BF), pltpu.VMEM((2 * slabs, slab, cols), BF),
            pltpu.VMEM(slab_shape, F32), pltpu.VMEM(slab_shape, BF), pltpu.VMEM(slab_shape, BF),
            pltpu.VMEM(slab_shape, F32), pltpu.VMEM((2, seq, units), BF),
            pltpu.VMEM((2, seq, units), BF), pltpu.VMEM((own, cols), F32),
            pltpu.VMEM((own, cols), F32), pltpu.VMEM((2, waves // 2, wave, cols), BF),
            pltpu.VMEM((2, waves // 2, wave, cols), BF), pltpu.VMEM((2 * slabs, slab, cols), BF),
            pltpu.VMEM((2, cols // rows, rows, cols), BF),
            pltpu.VMEM((2, units // rows, rows, cols), BF),
            dma((Gather.SEMS, n)), dma((Gather.SEMS, n)), dma((9,))]
        + Cross.sems() + Cross.sems() + [dma((8, PIECES)), dma((8, PIECES))],
        compiler_params=pltpu.CompilerParams(collective_id=1, **COMM), name="forward",
    )(patches, out_grad, *shards_in, flags, bias, vectors, small)


def tail(bias, qkv, do, ctx, lse, g_out, g_up, g_down, rows_out, weights, normed, block_in,
         grad_res, flags, gain, small):
    slots, _, heads, _, seq = qkv.shape
    rows, cols = g_out.shape[3:]
    wide = weights.shape[1]
    counts = [g_out.shape[2], g_up.shape[2], g_down.shape[2], wide // (4 * rows)]
    n = sum(counts)
    late = n - counts[3]
    block = 256
    parts = seq // block
    steps = slots * heads * parts
    own_rows = seq // 2
    slab = 128
    slabs = own_rows // slab
    hops = 5

    def kernel(bias_ref, qkv_ref, do_ref, ctx_ref, lse_ref, w_ref, n_ref, x_ref, res_ref,
               flags_ref, gain_ref, small_ref, go, gu, gd, y_ref,
               gp_ref, small_out, fo, fu, fd, fq, y_out, p_out,
               dk_ref, dv_ref, dqkv, gn1, given, taken, sums, incoming, stage, y_buf, p_buf,
               g_send, g_recv, s_send, s_recv, y_send, y_recv, p_send, p_recv, *scratch):
        step = pl.program_id(0)
        me = Me()
        reduce = Reduce(me, scratch)
        cross = Cross(me, y_ref, y_buf, y_send, y_recv)
        home_rows = Cross(me, stage, p_buf, p_send, p_recv)
        t_odd = lax.axis_index("tp") % 2

        def hand(i):
            return pltpu.make_async_remote_copy(
                src_ref=given.at[i], dst_ref=taken.at[i], send_sem=g_send.at[i],
                recv_sem=g_recv.at[i], device_id=me.core, device_id_type=MESH)

        partner = [me.core, me.x, me.y, me.near, me.two]

        def hop(k):
            return pltpu.make_async_remote_copy(
                src_ref=sums.at[k], dst_ref=incoming.at[k], send_sem=s_send.at[k],
                recv_sem=s_recv.at[k], device_id=partner[k], device_id_type=MESH)

        @pl.when(step == 0)
        def _():
            srcs = [go, gu, gd]
            reduce.load(srcs, lambda cp: cp.start())
            me.greet(two=True)
            reduce.load(srcs, lambda cp: cp.wait())
            reduce.prologue()

        reduce.tick(step)

        @pl.when(step < PIECES)
        def _():
            cross.start(step)

        part = step % parts
        head = step // parts
        slot, at_head = head // heads, head % heads
        at = pl.ds(pl.multiple_of(part * block, block), block)

        def feature(i):
            return pl.ds(pl.multiple_of((i * heads + at_head) * HEAD_DIM, HEAD_DIM), HEAD_DIM)

        k, v = qkv_ref[0, 1, 0], qkv_ref[0, 2, 0]
        q = qkv_ref[0, 0, 0, :, at] * jnp.asarray(HEAD_DIM ** (-0.5), BF)
        dob = do_ref[0, 0, :, at]
        inner = jnp.sum(dob.astype(F32) * ctx_ref[0, 0, :, at].astype(F32), 0, keepdims=True)
        scores = dg(jnp.concatenate([k, bias_ref[...]], 0),
                    jnp.concatenate([q, first_row(block)], 0), 0, 0)
        probs = jnp.exp(scores - lse_ref[0, 0, :, at])
        ds = (probs * (dg(v, dob, 0, 0) - inner)).astype(BF)
        first = part == 0
        dv = dg(dob, probs.astype(BF), 1, 1)
        dk = dg(q, ds, 1, 1)
        dqkv[slot, feature(0), at] = (dg(k, ds, 1, 0) * HEAD_DIM ** (-0.5)).astype(BF)

        @pl.when(first)
        def _():
            dk_ref[...] = dk
            dv_ref[...] = dv

        @pl.when(jnp.logical_not(first))
        def _():
            dk_ref[...] += dk
            dv_ref[...] += dv

        @pl.when(part == parts - 1)
        def _():
            dqkv[slot, feature(1), :] = dk_ref[...].astype(BF)
            dqkv[slot, feature(2), :] = dv_ref[...].astype(BF)

        @pl.when(step == steps - 1)
        def _():
            clock = [steps]

            def tick():
                reduce.tick(jnp.int32(clock[0]))
                clock[0] += 1

            quarter = wide // 4
            for s in range(2):
                def piece(i, carry, s=s):
                    at_rows = pl.ds(pl.multiple_of(i * quarter, 16), quarter)
                    out = dg(dqkv[s, at_rows, :], n_ref[...], 1, 0)
                    reduce.g[s, i, late:] = out.astype(BF).reshape(counts[3], rows, cols)
                    return carry
                lax.fori_loop(0, 4, piece, 0)
                if s == 0:
                    tick()
            sums[0] = small_ref[...]
            ones = jnp.ones((8, seq), BF)
            third = wide // 3
            for s in range(2):
                line = dg(ones, dqkv[s], 1, 1)[0:1]
                line = jnp.concatenate(
                    [line[:, :third], line[:, 2 * third:],
                     jnp.zeros((1, cols - 2 * third), F32)], 1)
                where = 1 + 2 * me.c + (t_odd if s == 0 else 1 - t_odd)
                sums[0, where, 1:2, :] = line

            def partial(low):
                at_rows = pl.ds(pl.multiple_of(low, slab), slab)
                return dg(dqkv[0, :, at_rows], w_ref[0], 0, 0) + dg(dqkv[1, :, at_rows], w_ref[1], 0, 0)

            def other_half(i, carry):
                given[i] = partial(own_rows + i * slab).astype(BF)
                hand(i).start()
                reduce.tick(steps + 1 + i)
                return carry
            lax.fori_loop(0, slabs, other_half, 0)

            def own_half(i, carry):
                gn1[i] = partial(i * slab)
                reduce.tick(steps + 1 + slabs + i)
                return carry
            lax.fori_loop(0, slabs, own_half, 0)

            def norm_back(i, carry):
                d_mask, d_gain, d_bias = carry
                at_rows = pl.ds(pl.multiple_of(i * slab, slab), slab)
                hand(i).wait_recv()
                grad = gn1[i] + taken[i].astype(F32)
                value = x_ref[at_rows, :]
                center = value - jnp.mean(value, -1, keepdims=True)
                scale = lax.rsqrt(jnp.mean(center * center, -1, keepdims=True) + 1e-06)
                unit = center * scale
                turned = grad * gain_ref[0:1, :]
                inside = (turned - jnp.mean(turned, -1, keepdims=True)
                          - unit * jnp.mean(turned * unit, -1, keepdims=True))
                grad_in = res_ref[at_rows, :] + scale * inside
                valid = flag_rows(flags_ref, at_rows, 0, cols)
                masked = flag_rows(flags_ref, at_rows, 1, cols)
                kept = valid * (1.0 - masked) * grad_in
                gp_ref[at_rows, :] = kept
                stage[i] = kept.astype(BF)
                home_rows.start(i)
                reduce.tick(steps + 1 + 2 * slabs + i)
                total = lambda v: jnp.sum(v, 0, keepdims=True)
                return (d_mask + total(valid * masked * grad_in),
                        d_gain + total(grad * unit), d_bias + total(grad))
            zero = jnp.zeros((1, cols), F32)
            lines = lax.fori_loop(0, slabs, norm_back, (zero, zero, zero))
            for k in range(3):
                sums[0, 0, k:k + 1, :] = lines[k]
            hop(0).start()
            begin = steps + 1 + 3 * slabs

            def step_on(index, carry):
                reduce.tick(index)
                for k in range(hops):
                    @pl.when(index == begin + 3 * k + 2)
                    def _(k=k):
                        hop(k).wait_recv()
                        sums[k + 1] = sums[k] + incoming[k]
                        if k + 1 < hops:
                            hop(k + 1).start()
                return carry
            lax.fori_loop(begin, max(reduce.ticks, begin + 3 * hops), step_on, 0)
            small_out[...] = sums[hops]
            for i in range(PIECES):
                cross.wait(i)
                home_rows.wait(i)
            y_copy = pltpu.make_async_copy(y_buf, y_out, reduce.local.at[6])
            p_copy = pltpu.make_async_copy(p_buf, p_out, reduce.local.at[7])
            y_copy.start()
            p_copy.start()
            for k in range(hops):
                hop(k).wait_send()
            for i in range(slabs):
                hand(i).wait_send()
            cross.drain()
            home_rows.drain()
            reduce.finish([fo, fu, fd, fq])
            y_copy.wait()
            p_copy.wait()

    col, tri, one, row = head_specs(heads, seq, parts)
    pairs = slots * heads * seq * seq
    dma = pltpu.SemaphoreType.DMA
    vmem = pl.BlockSpec(memory_space=pltpu.VMEM)
    hand_shape = (slabs, slab, cols)
    return pl.pallas_call(
        kernel, grid=(steps,), in_specs=[col, tri, one, one, row] + [vmem] * 7 + [ANY] * 4,
        out_specs=[vmem, vmem] + [ANY] * 6,
        out_shape=[jax.ShapeDtypeStruct((own_rows, cols), F32), jax.ShapeDtypeStruct(small.shape, F32)]
        + [jax.ShapeDtypeStruct((4, k, rows, cols), BF) for k in counts]
        + [jax.ShapeDtypeStruct(rows_out.shape, BF)] * 2,
        scratch_shapes=[pltpu.VMEM((HEAD_DIM, seq), F32)] * 2
        + [pltpu.VMEM((2, wide, seq), BF), pltpu.VMEM(hand_shape, F32), pltpu.VMEM(hand_shape, BF),
           pltpu.VMEM(hand_shape, BF), pltpu.VMEM((hops + 1,) + small.shape, F32),
           pltpu.VMEM((hops,) + small.shape, F32)] + [pltpu.VMEM(rows_out.shape, BF)] * 3
        + [dma((slabs,)), dma((slabs,)), dma((hops,)), dma((hops,))] + Cross.sems() + Cross.sems()
        + Reduce.scratch(n, rows, cols),
        compiler_params=pltpu.CompilerParams(collective_id=3, **COMM), name="tail",
        cost_estimate=pl.CostEstimate(flops=pairs * 10 * HEAD_DIM, bytes_accessed=qkv.size * 6,
                                      transcendentals=pairs),
    )(bias, qkv, do, ctx, lse, weights, normed, block_in, grad_res, flags, gain, small,
      g_out, g_up, g_down, rows_out)


def rest(w, total):
    if w.n_dp > 8:
        groups = [[r + 8 * g for g in range(w.n_dp // 8)] for r in range(8)]
        total = lax.psum(total, "dp", axis_index_groups=groups)
    return total


class Wires:
    def __init__(self, n_dp, n_tp):
        assert n_tp == 4 and n_dp % 8 == 0
        self.n_dp, self.n_tp = n_dp, n_tp
        self.core = [(d * n_tp + t, (d ^ 1) * n_tp + t) for d in range(n_dp) for t in range(n_tp)]

    def other(self, value):
        return lax.ppermute(value, AXES, self.core)


def shards(w, patches, validity, mask_pos, mask_token, ln1_gain, ln1_bias, w_qkv, b_qv, w_out,
           b_out, ln2_gain, ln2_bias, w_up, b_up, w_down, b_down, out_grad):
    d, t = lax.axis_index("dp"), lax.axis_index("tp")
    c = d & 1
    rows, width = patches.shape
    seq = validity.shape[1]
    local = w_qkv.shape[2]
    heads = local // HEAD_DIM
    wide = 3 * local
    swapped = ((d ^ t) & 1) == 1
    pieces = lambda v: v.reshape(PIECES, rows // PIECES, width)
    chunk = lambda v, k: v.reshape(v.shape[:-2] + (4, -1, k, width))

    bucket = t >> 1
    flags = jnp.stack([lax.dynamic_index_in_dim(validity, bucket, 0, False),
                       lax.dynamic_index_in_dim(mask_pos, bucket, 0, False)])
    flags = jnp.where(swapped, w.other(flags), flags)
    own_flags = lax.dynamic_slice_in_dim(flags, c * rows, rows, 1)
    other_flags = lax.dynamic_slice_in_dim(flags, (1 - c) * rows, rows, 1)
    valid_row = jnp.concatenate([own_flags[0], other_flags[0]]).astype(BF)[None]
    mask_row = jnp.concatenate([own_flags[1], other_flags[1]]).astype(BF)[None]
    empty = jnp.zeros((14, seq), BF)
    flags = jnp.concatenate([valid_row, mask_row, empty])
    key_bias = jnp.concatenate(
        [((valid_row.astype(F32) - 1.0) * 1000000000.0).astype(BF), empty, empty[:1]])
    vectors = jnp.stack([mask_token, ln1_gain, ln1_bias, b_out, ln2_gain, ln2_bias, b_down, b_down])
    line = jnp.concatenate([b_qv[0], jnp.zeros((local,), F32), b_qv[1],
                            jnp.zeros((width - wide,), F32)])
    small = jnp.concatenate([b_up[None], line[None], jnp.zeros((6, width), F32)])
    turned = w_qkv.transpose(1, 2, 0).reshape(wide, width)
    (wq, normed_all, qkv, context, log_norm, grad_context, block_in, grad_res, output, small, g_out,
     g_up, g_down) = forward(
        pieces(patches), pieces(out_grad),
        [chunk(turned, CHUNK), chunk(w_out, CHUNK), chunk(w_up, CHUNK), chunk(w_down, CHUNK)],
        flags, key_bias, vectors, small)
    by_head = lambda v: v.reshape(2, heads, HEAD_DIM, seq)
    fours = lambda v: v.reshape(2, 4, -1, CHUNK, width)
    grad_patches, totals, f_out, f_up, f_down, f_qkv, output, moved = tail(
        key_bias, qkv.reshape(2, 3, heads, HEAD_DIM, seq), by_head(grad_context), by_head(context),
        log_norm.reshape(2, heads, 1, seq), fours(g_out), fours(g_up), fours(g_down), output,
        wq.reshape(2, wide, width), normed_all.reshape(seq, width), block_in, grad_res, flags,
        vectors[1:2], small)
    output = output.reshape(rows, width)
    grad_patches = jnp.where(swapped, moved.reshape(rows, width).astype(F32), grad_patches)
    totals = rest(w, totals)
    mine = lax.dynamic_index_in_dim(totals, 1 + t, 0, False)
    totals = totals[0]
    whole = lambda v: rest(w, v.reshape(-1, width).astype(F32))
    grad_w_qkv = whole(f_qkv).reshape(3, local, width).transpose(2, 0, 1)
    return (output, grad_patches, totals[0], totals[1], totals[2], grad_w_qkv,
            mine[1, :2 * local].reshape(2, local), whole(f_out), totals[3], totals[4], totals[5],
            whole(f_up), mine[0], whole(f_down), totals[6])


def solution(mesh):
    w = Wires(mesh.shape["dp"], mesh.shape["tp"])
    rows, cols = P(AXES, None), P(None, "tp")
    return jax.shard_map(
        lambda *args: shards(w, *args),
        mesh=mesh,
        in_specs=(rows, P("dp", None), P("dp", None), P(), P(), P(), P(None, None, "tp"), cols,
                  P("tp", None), P(), P(), P(), cols, P("tp"), P("tp", None), P(), rows),
        out_specs=(rows, rows, P(), P(), P(), P(None, None, "tp"), cols, P("tp", None), P(), P(),
                   P(), cols, P("tp"), P("tp", None), P()),
        check_vma=False,
    )
```

```python
import jax
import jax.numpy as jnp
from jax import lax
from jax.experimental import pallas as pl
from jax.experimental.pallas import tpu as pltpu
from jax.sharding import PartitionSpec as P

HEAD_DIM = 64
GAP_GATHER = 4
GAP_REDUCE = 5
HOP = 2
TALL = 256
PIECES = 4
CHUNK = 16
AXES = ("dp", "tp")
BF = jnp.bfloat16
F32 = jnp.float32


def dg(left, right, ldim, rdim):
    return lax.dot_general(left, right, (((ldim,), (rdim,)), ((), ())), preferred_element_type=F32)


def first_row(block):
    return jnp.where(lax.broadcasted_iota(jnp.int32, (16, block), 0) < 1, 1.0, 0.0).astype(BF)


class Me:
    def __init__(self):
        d, t = lax.axis_index("dp"), lax.axis_index("tp")
        c, qx, qy = d % 2, (d // 2) % 2, (d // 4) % 2
        self.c = c
        self.home = (t // 2 + c + 1) % 2
        self.swapped = (d + t) % 2
        self.core = {"dp": d + 1 - 2 * c, "tp": t}
        self.x = {"dp": d + 2 - 4 * qx, "tp": t}
        self.y = {"dp": d + 4 - 8 * qy, "tp": t}
        self.near = {"dp": d, "tp": t + 1 - 2 * (t % 2)}
        self.far = {"dp": d + 1 - 2 * c, "tp": 2 * c + t % 2}
        self.cross = {"dp": d + 1 - 2 * c, "tp": t + 1 - 2 * (t % 2)}
        self.two = {"dp": d, "tp": t + 2 - 4 * (t // 2)}
        self.q = [qx + 2 * qy, 1 - qx + 2 * qy, qx + 2 * (1 - qy), 1 - qx + 2 * (1 - qy)]

    def greet(self, swap=True, two=False):
        barrier = pltpu.get_barrier_semaphore()
        others = [self.core, self.x, self.y, self.near] + ([self.two] if two else [])
        for other in others:
            pl.semaphore_signal(barrier, inc=1, device_id=other, device_id_type=MESH)

        @pl.when(self.home == 0)
        def _():
            pl.semaphore_signal(barrier, inc=1, device_id=self.far, device_id_type=MESH)

        if swap:
            @pl.when(self.swapped == 1)
            def _():
                pl.semaphore_signal(barrier, inc=1, device_id=self.cross, device_id_type=MESH)

        extra = self.swapped if swap else 0
        pl.semaphore_wait(barrier, len(others) + 1 - self.home + extra)


class Cross:
    @staticmethod
    def sems():
        return [pltpu.SemaphoreType.DMA((PIECES,)), pltpu.SemaphoreType.DMA((PIECES,))]

    def __init__(self, me, src, dst, send, recv):
        self.me, self.src, self.dst, self.send, self.recv = me, src, dst, send, recv

    def copy(self, i):
        return pltpu.make_async_remote_copy(
            src_ref=self.src.at[i], dst_ref=self.dst.at[i], send_sem=self.send.at[i],
            recv_sem=self.recv.at[i], device_id=self.me.cross, device_id_type=MESH)

    def keep(self, i):
        return pltpu.make_async_copy(self.src.at[i], self.dst.at[i], self.recv.at[i])

    def start(self, i):
        @pl.when(self.me.swapped == 1)
        def _():
            self.copy(i).start()

        @pl.when(self.me.swapped == 0)
        def _():
            self.keep(i).start()

    def wait(self, i):
        @pl.when(self.me.swapped == 1)
        def _():
            self.copy(i).wait_recv()

        @pl.when(self.me.swapped == 0)
        def _():
            self.keep(i).wait()

    def drain(self):
        @pl.when(self.me.swapped == 1)
        def _():
            for i in range(PIECES):
                self.copy(i).wait_send()


class Gather:
    STAGES = 4
    SEMS = 6

    def __init__(self, me, srcs, full, send, recv, local):
        self.me, self.srcs, self.full, self.send, self.recv = me, srcs, full, send, recv
        self.local = local
        self.n = full.shape[2]
        self.spans = spans(srcs)

    def keep_own(self, act):
        @pl.when(self.me.home == 1)
        def _():
            for i, (src, (low, high)) in enumerate(zip(self.srcs, self.spans)):
                act(pltpu.make_async_copy(src, self.full.at[0, :, pl.ds(low, high - low)],
                                          self.local.at[i]))

    def copy(self, kind, n, src, dst, device):
        return pltpu.make_async_remote_copy(
            src_ref=src, dst_ref=dst, send_sem=self.send.at[kind, n],
            recv_sem=self.recv.at[kind, n], device_id=device, device_id_type=MESH)

    def pull(self, n, home, src=None):
        me, q = self.me, self.me.q[0]
        slot = 1 if home else 0
        src = self.full.at[slot, q, n] if src is None else src
        return self.copy(0, n, src, self.full.at[slot, q, n], me.near if home else me.far)

    def relay(self, n):
        q = self.me.q[0]
        return self.copy(1, n, self.full.at[0, q, n], self.full.at[1, q, n], self.me.near)

    def plane(self, n, home):
        q, first = self.me.q[0], (1 if home else 0)
        part = self.full.at[pl.ds(first, 2 - first), q, n]
        return [self.copy(2, n, part, part, self.me.x), self.copy(3, n, part, part, self.me.y)]

    def diag(self, n, slot, through_x):
        if through_x:
            part = self.full.at[slot, self.me.q[2], n]
            return self.copy(4, n, part, part, self.me.x)
        part = self.full.at[slot, self.me.q[1], n]
        return self.copy(5, n, part, part, self.me.y)

    def diags(self, n, home, act):
        if home:
            @pl.when(n % 2 == 0)
            def _():
                act(self.diag(n, 1, True))

            @pl.when(n % 2 == 1)
            def _():
                act(self.diag(n, 1, False))
        else:
            act(self.diag(n, 0, True))
            act(self.diag(n, 1, False))

    def sides(self, body):
        @pl.when(self.me.home == 1)
        def _():
            body(True)

        @pl.when(self.me.home == 0)
        def _():
            body(False)

    def start(self, n):
        @pl.when(n < self.n)
        def _():
            for src, (low, high) in zip(self.srcs, self.spans):
                @pl.when(jnp.logical_and(n >= low, n < high))
                def _(src=src, low=low):
                    part = src.at[self.me.q[0], n - low]
                    self.sides(lambda home: self.pull(n, home, part).start())

    def prologue(self):
        self.start(jnp.int32(0))
        self.start(jnp.int32(1))

    def tick(self, step):
        def stage(n, body):
            @pl.when(jnp.logical_and(n >= 0, n < self.n))
            def _():
                body(n)

        def four(n):
            self.sides(lambda home: self.diags(n, home, lambda c: c.wait_recv()))

        def three(n):
            def side(home):
                for c in self.plane(n, home):
                    c.wait_recv()
                self.diags(n, home, lambda c: c.start())
            self.sides(side)

        def two(n):
            def side(home):
                if not home:
                    self.relay(n).wait_recv()
                for c in self.plane(n, home):
                    c.start()
            self.sides(side)

        def one(n):
            def side(home):
                self.pull(n, home).wait_recv()
                if not home:
                    self.relay(n).start()
            self.sides(side)

        for index, body in reversed(list(enumerate([one, two, three, four]))):
            stage(step - 1 - GAP_GATHER * index, body)
        self.start(step + 2)

    @property
    def ticks(self):
        return self.n + 1 + GAP_GATHER * (self.STAGES - 1)

    def finish(self):
        def drain(n, carry):
            def side(home):
                self.pull(n, home).wait_send()
                if not home:
                    self.relay(n).wait_send()
                for c in self.plane(n, home):
                    c.wait_send()
                self.diags(n, home, lambda c: c.wait_send())
            self.sides(side)
            return carry
        lax.fori_loop(0, self.n, drain, 0)

    def write(self, outs, act):
        for i, (out, (low, high)) in enumerate(zip(outs, self.spans)):
            act(pltpu.make_async_copy(self.full.at[:, :, pl.ds(low, high - low)], out,
                                      self.local.at[i]))


class Reduce:
    STAGES = 8
    SEMS = 11

    @staticmethod
    def scratch(n, rows, cols):
        piece = (rows, cols)
        return [
            pltpu.VMEM((2, 4, n) + piece, BF), pltpu.VMEM((n,) + piece, BF),
            pltpu.VMEM((n,) + piece, BF), pltpu.VMEM((2, n) + piece, BF),
            pltpu.VMEM((2, n) + piece, BF), pltpu.VMEM((n,) + piece, BF),
            pltpu.VMEM((n,) + piece, BF), pltpu.VMEM((n,) + piece, BF),
            pltpu.VMEM((n,) + piece, F32),
            pltpu.VMEM((4, n) + piece, BF),
            pltpu.SemaphoreType.DMA((Reduce.SEMS, n)), pltpu.SemaphoreType.DMA((Reduce.SEMS, n)),
            pltpu.SemaphoreType.DMA((12,)),
        ]

    def __init__(self, me, refs, early, bubble):
        (self.g, self.ax, self.by, self.tx, self.ty, self.back, self.got, self.take,
         self.acc, self.fin, self.send, self.recv, self.local) = refs
        self.me, self.early, self.bubble = me, early, bubble
        self.n = self.g.shape[2]

    def copy(self, kind, n, src, dst, device):
        return pltpu.make_async_remote_copy(
            src_ref=src, dst_ref=dst, send_sem=self.send.at[kind, n],
            recv_sem=self.recv.at[kind, n], device_id=device, device_id_type=MESH)

    def corner(self, n):
        q = self.me.q[3]
        return [self.copy(0, n, self.g.at[0, q, n], self.ax.at[n], self.me.x),
                self.copy(1, n, self.g.at[1, q, n], self.by.at[n], self.me.y)]

    def side(self, n):
        q = self.me.q
        return [self.copy(2, n, self.g.at[:, q[1], n], self.tx.at[:, n], self.me.x),
                self.copy(3, n, self.g.at[:, q[2], n], self.ty.at[:, n], self.me.y)]

    def second(self, n):
        return self.copy(4, n, self.g.at[1, self.me.q[0], n], self.back.at[n], self.me.near)

    def push(self, n, home):
        q = self.me.q[0]
        if home:
            return self.copy(5, n, self.g.at[1, q, n], self.got.at[n], self.me.near)
        return self.copy(5, n, self.g.at[0, q, n], self.got.at[n], self.me.far)

    def pair(self, n):
        return self.copy(6, n, self.back.at[n], self.take.at[n], self.me.core)

    def spread(self, n):
        part = self.fin.at[self.me.q[0], n]
        return [self.copy(7, n, part, part, self.me.x), self.copy(8, n, part, part, self.me.y)]

    def diag(self, n, act):
        @pl.when(n // 2 % 2 == 0)
        def _():
            part = self.fin.at[self.me.q[2], n]
            act(self.copy(9, n, part, part, self.me.x))

        @pl.when(n // 2 % 2 == 1)
        def _():
            part = self.fin.at[self.me.q[1], n]
            act(self.copy(9, n, part, part, self.me.y))

    def share(self, n):
        part = self.fin.at[:, n]
        return self.copy(10, n, part, part, self.me.core)

    def owner(self, n, body):
        pl.when((n + self.me.c) % 2 == 0)(body)

    def helper(self, n, body):
        pl.when((n + self.me.c) % 2 == 1)(body)

    def live(self, n, body):
        late = self.early + self.bubble
        here = jnp.logical_or(n < self.early, jnp.logical_and(n >= late, n < self.n + self.bubble))

        @pl.when(jnp.logical_and(n >= 0, here))
        def _():
            body(jnp.minimum(n, self.early - 1) + jnp.maximum(n - (late - 1), 0))

    def start(self, n):
        def begin(n):
            for c in self.corner(n):
                c.start()
        self.live(n, begin)

    def tick(self, step):
        me, g, acc = self.me, self.g, self.acc
        q, c = me.q, me.c
        home_f = me.home.astype(F32)

        def away(body):
            pl.when(me.home == 0)(body)

        def at_home(body):
            pl.when(me.home == 1)(body)

        def eight(n):
            self.helper(n, lambda: self.share(n).wait_recv())

        def seven(n):
            def own():
                self.diag(n, lambda cp: cp.wait_recv())
                self.share(n).start()
            self.owner(n, own)

        def six(n):
            def own():
                for cp in self.spread(n):
                    cp.wait_recv()
                self.diag(n, lambda cp: cp.start())
            self.owner(n, own)

        def five(n):
            def own():
                self.pair(n).wait_recv()
                self.fin[q[0], n] = (acc[n] + self.take[n].astype(F32)).astype(BF)
                for cp in self.spread(n):
                    cp.start()
            self.owner(n, own)

        def four(n):
            at_home(lambda: self.push(n, True).wait_recv())
            away(lambda: self.push(n, False).wait_recv())
            total = acc[n] * home_f + self.got[n].astype(F32)

            def own():
                acc[n] = total

            def help_out():
                self.back[n] = total.astype(BF)
                self.pair(n).start()
            self.owner(n, own)
            self.helper(n, help_out)

        def three(n):
            def side():
                self.second(n).wait_recv()
                g[0, q[0], n] = (acc[n] + self.back[n].astype(F32)).astype(BF)
                self.push(n, False).start()
            away(side)

        def two(n):
            for cp in self.side(n):
                cp.wait_recv()
            g[1, q[0], n] = (g[1, q[0], n].astype(F32) + self.tx[1, n].astype(F32)
                             + self.ty[1, n].astype(F32)).astype(BF)
            away(lambda: self.second(n).start())
            at_home(lambda: self.push(n, True).start())
            acc[n] = (g[0, q[0], n].astype(F32) + self.tx[0, n].astype(F32)
                      + self.ty[0, n].astype(F32))

        def one(n):
            for cp in self.corner(n):
                cp.wait_recv()
            g[1, q[1], n] = (g[1, q[1], n].astype(F32) + self.by[n].astype(F32)).astype(BF)
            g[0, q[2], n] = (g[0, q[2], n].astype(F32) + self.ax[n].astype(F32)).astype(BF)
            for cp in self.side(n):
                cp.start()

        bodies = [one, two, three, four, five, six, seven, eight]
        for index in reversed(range(8)):
            self.live(step - 1 - GAP_REDUCE * index, bodies[index])
        self.start(step + 2)

    @property
    def ticks(self):
        return self.n + self.bubble + 1 + GAP_REDUCE * (self.STAGES - 1)

    def finish(self, outs):
        def drain(n, carry):
            for cp in self.corner(n) + self.side(n):
                cp.wait_send()

            @pl.when(self.me.home == 1)
            def _():
                self.push(n, True).wait_send()

            @pl.when(self.me.home == 0)
            def _():
                self.second(n).wait_send()
                self.push(n, False).wait_send()

            def own():
                for cp in self.spread(n) + [self.share(n)]:
                    cp.wait_send()
                self.diag(n, lambda cp: cp.wait_send())
            self.owner(n, own)
            self.helper(n, lambda: self.pair(n).wait_send())
            return carry
        lax.fori_loop(0, self.n, drain, 0)
        copies = [pltpu.make_async_copy(self.fin.at[:, pl.ds(low, count)], out, self.local.at[i])
                  for i, (low, count, out) in enumerate(outs)]
        for cp in copies:
            cp.start()
        for cp in copies:
            cp.wait()


def spans(srcs):
    result, low = [], 0
    for src in srcs:
        result.append((low, low + src.shape[1]))
        low += src.shape[1]
    return result


MESH = pl.DeviceIdType.MESH
COMM = dict(has_side_effects=True, vmem_limit_bytes=66500000)
ANY = pl.BlockSpec(memory_space=pl.ANY)


def stats(value):
    center = value - jnp.mean(value, -1, keepdims=True)
    scale = lax.rsqrt(jnp.mean(center * center, -1, keepdims=True) + 1e-06)
    return center, scale


def flag_rows(flags_ref, at, which, cols):
    pick = jnp.where(lax.broadcasted_iota(jnp.int32, (16, cols), 0) == which, 1.0, 0.0)
    return dg(flags_ref[:, at], pick.astype(BF), 0, 0)


def total_rows(value):
    return jnp.sum(value, 0, keepdims=True)


def layer(patches, out_grad, shards_in, flags, b_qv, b_up, vectors):
    rows, cols = shards_in[0].shape[2:]
    counts = [v.shape[1] for v in shards_in]
    n = sum(counts)
    piece = patches.shape[1]
    own = PIECES * piece
    seq = 2 * own
    slab = 128
    slabs = own // slab
    wide = 4 * rows * counts[0]
    local = 4 * rows * counts[1]
    units = 4 * rows * counts[3]
    third = wide // 3
    heads = local // HEAD_DIM
    low = [sum(counts[:i]) for i in range(5)]
    block = 512
    parts = seq // block
    wave = 256
    waves = seq // wave
    span = 256
    spans_of = units // span
    per = span // (4 * rows)
    early = 2 * per * spans_of + counts[1]
    narrow = 256
    narrow_parts = seq // narrow
    bubble = 2 * heads * narrow_parts
    chunks = early + counts[0]
    hops = 5

    def kernel(x_ref, y_ref, s0, s1, s2, s3, flags_ref, qv_ref, up_ref, l0, l1, l2, l3, l4,
               l5, l6,
               gp_out, small_out, fo, fu, fd, fq, out_out, p_out,
               x_buf, y_buf, normed, small_buf, full, second, given, taken, residual, block_ref,
               hidden, grad_pre, mlp_sum, gn2_sum, gres, qkv_ref, ctx_ref, lse_ref, do_ref,
               out_rows, out_buf, stage, p_buf, dk_ref, dv_ref, sums, incoming,
               vec_ref, small_ref, bias_ref, send, recv, local_sem, x_send, x_recv, y_send, y_recv, o_send, o_recv, p_send, p_recv,
               hand_send, hand_recv, *scratch):
        me = Me()
        srcs = [s0, s1, s2, s3]
        gather = Gather(me, srcs, full, send, recv, local_sem)
        cross_x = Cross(me, x_ref, x_buf, x_send, x_recv)
        cross_y = Cross(me, y_ref, y_buf.at[pl.ds(0, PIECES)], y_send, y_recv)
        cross_out = Cross(me, out_rows, out_buf, o_send, o_recv)
        cross_p = Cross(me, stage, p_buf, p_send, p_recv)
        reduce = Reduce(me, scratch, early, bubble)
        t_odd = lax.axis_index("tp") % 2

        def hand(kind, i, src, dst):
            return pltpu.make_async_remote_copy(
                src_ref=src, dst_ref=dst, send_sem=hand_send.at[kind, i],
                recv_sem=hand_recv.at[kind, i], device_id=me.core, device_id_type=MESH)

        def hand_n1(i):
            return hand(0, i, normed.at[0, i], normed.at[1, i])

        def hand_y(i):
            return hand(1, i, y_buf.at[i], y_buf.at[PIECES + i])

        def hand_attn(i):
            return hand(2, i, given.at[0, i], taken.at[0, i])

        def hand_n2(i):
            return hand(3, i, second.at[i], second.at[slabs + i])

        def hand_mlp(i):
            return hand(4, i, given.at[1, i], taken.at[1, i])

        def hand_gn2(i):
            return hand(5, i, given.at[0, i], taken.at[0, i])

        def hand_res(i):
            return hand(6, i, gres.at[i], gres.at[slabs + i])

        def hand_gn1(i):
            return hand(8, i, given.at[1, i], taken.at[1, i])

        partner = [me.core, me.x, me.y, me.near, me.two]

        def hop(k, turn):
            return pltpu.make_async_remote_copy(
                src_ref=sums.at[turn, k], dst_ref=incoming.at[turn, k],
                send_sem=hand_send.at[9 + k, turn], recv_sem=hand_recv.at[9 + k, turn],
                device_id=partner[k], device_id_type=MESH)

        def hop_on(k, turn):
            hop(k, turn).wait_recv()
            sums[turn, k + 1] = sums[turn, k] + incoming[turn, k]
            if k + 1 < hops:
                hop(k + 1, turn).start()

        def bias_pull(at_home):
            return pltpu.make_async_remote_copy(
                src_ref=small_ref, dst_ref=small_buf.at[1 if at_home else 0],
                send_sem=hand_send.at[7, 0], recv_sem=hand_recv.at[7, 0],
                device_id=me.near if at_home else me.far, device_id_type=MESH)

        bias_relay = pltpu.make_async_remote_copy(
            src_ref=small_buf.at[0], dst_ref=small_buf.at[1], send_sem=hand_send.at[7, 1],
            recv_sem=hand_recv.at[7, 1], device_id=me.near, device_id_type=MESH)
        bias_keep = pltpu.make_async_copy(small_ref, small_buf.at[0], local_sem.at[4])

        def home(body):
            pl.when(me.home == 1)(body)

        def away(body):
            pl.when(me.home == 0)(body)

        def at_slab(i, size=slab):
            return pl.ds(pl.multiple_of(i * size, size), size)

        def weight(slot, which):
            part = full[slot, :, low[which]:low[which + 1]]
            return part.reshape(4 * rows * counts[which], cols)

        for k, line in enumerate((l0, l1, l2, l3, l4, l5, l6)):
            vec_ref[k:k + 1, :] = line[...].reshape(1, cols)
        gap = jnp.zeros((1, local), F32)
        small_ref[...] = jnp.zeros(small_ref.shape, F32)
        small_ref[0:1, :] = up_ref[...].reshape(1, cols)
        small_ref[1:2, :] = jnp.concatenate(
            [qv_ref[0:1, :], gap, qv_ref[1:2, :], jnp.zeros((1, cols - wide), F32)], 1)
        bias_ref[...] = ((flags_ref[...].astype(F32) - 1.0) * 1000000000.0).astype(BF)
        me.greet(two=True)
        gather.keep_own(lambda cp: cp.start())
        home(lambda: bias_keep.start())
        home(lambda: bias_pull(True).start())
        away(lambda: bias_pull(False).start())
        gather.prologue()
        cross_x.start(0)
        cross_x.start(1)
        gather.keep_own(lambda cp: cp.wait())

        def first_norm(i):
            at = at_slab(i, piece)
            valid = flag_rows(flags_ref, at, 0, cols)
            masked = flag_rows(flags_ref, at, 1, cols)
            value = (valid * (1.0 - masked) * x_buf[i].astype(F32)
                     + valid * masked * vec_ref[0:1, :])
            block_ref[at, :] = value
            center, scale = stats(value)
            normed[0, i] = (center * scale * vec_ref[1:2, :] + vec_ref[2:3, :]).astype(BF)

        def step(index, carry):
            gather.tick(index)

            @pl.when(index < PIECES - 2)
            def _():
                cross_x.start(index + 2)

            @pl.when(jnp.logical_and(index >= 1, index < PIECES + 1))
            def _():
                cross_x.wait(index - 1)
                first_norm(index - 1)
                hand_n1(index - 1).start()

            @pl.when(index == 4)
            def _():
                def relay():
                    bias_pull(False).wait_recv()
                    bias_relay.start()
                away(relay)
            return carry
        clock = max(counts[0] + 1 + 3 * GAP_GATHER, PIECES + 1)
        lax.fori_loop(0, clock, step, 0)
        for i in range(PIECES):
            hand_n1(i).wait_recv()

        def own_bias():
            bias_keep.wait()
            bias_pull(True).wait_recv()
        home(own_bias)
        away(lambda: bias_relay.wait_recv())
        rows_all = normed[...].reshape(seq, cols)
        ones = jnp.where(lax.broadcasted_iota(jnp.int32, (16, seq), 0) < 2, 1.0, 0.0).astype(BF)
        for slot in range(2):
            line = small_buf[slot, 1:2, :]
            high = line.astype(BF)
            rest_of = (line - high.astype(F32)).astype(BF)
            pair = jnp.concatenate([high, rest_of, jnp.zeros((14, cols), BF)], 0)[:, :wide]
            weights = weight(slot, 0)
            for part in range(3):
                at = slice(part * third, part * third + third)
                out = dg(weights[at], rows_all, 1, 1) + dg(pair[:, at], ones, 0, 0)
                qkv_ref[slot, at] = out.astype(BF)

        def attention(index, carry):
            gather.tick(clock + index)

            @pl.when(index >= 2 * heads * parts - PIECES)
            def _():
                cross_y.start(index - (2 * heads * parts - PIECES))

            head = index // parts
            slot, at_head = head // heads, head % heads

            def feature(i):
                return pl.ds(pl.multiple_of((i * heads + at_head) * HEAD_DIM, HEAD_DIM), HEAD_DIM)

            at = at_slab(index % parts, block)
            k, v = qkv_ref[slot, feature(1), :], qkv_ref[slot, feature(2), :]
            q = qkv_ref[slot, feature(0), at] * jnp.asarray(HEAD_DIM ** (-0.5), BF)
            scores = dg(jnp.concatenate([k, bias_ref[...]], 0),
                        jnp.concatenate([q, first_row(block)], 0), 0, 0)
            top = jnp.max(scores, 0, keepdims=True)
            powered = jnp.exp(scores - top)
            summed = jnp.concatenate([v, jnp.ones((16, seq), BF)], 0)
            out = dg(summed, powered.astype(BF), 1, 0)
            total = out[HEAD_DIM:HEAD_DIM + 1]
            ctx_ref[pl.ds(pl.multiple_of(head * HEAD_DIM, HEAD_DIM), HEAD_DIM), at] = (
                out[:HEAD_DIM] / total).astype(BF)
            lse_ref[head, :, at] = top + jnp.log(total)
            return carry
        lax.fori_loop(0, 2 * heads * parts, attention, 0)
        clock = clock + 2 * heads * parts

        def projected(i):
            at = at_slab(i)
            return (dg(ctx_ref[0:local, at], weight(0, 1), 0, 0)
                    + dg(ctx_ref[local:2 * local, at], weight(1, 1), 0, 0))

        def other_half(i, carry):
            given[0, i] = projected(slabs + i).astype(BF)
            hand_attn(i).start()
            gather.tick(clock + i)
            return carry
        lax.fori_loop(0, slabs, other_half, 0)

        def own_half(i, carry):
            mlp_sum[at_slab(i), :] = projected(i)
            gather.tick(clock + slabs + i)
            return carry
        lax.fori_loop(0, slabs, own_half, 0)

        def second_norm(i, carry):
            hand_attn(i).wait_recv()
            value = (block_ref[at_slab(i), :] + mlp_sum[at_slab(i), :] + taken[0, i].astype(F32)
                     + vec_ref[3:4, :])
            residual[i] = value
            center, scale = stats(value)
            second[i] = (center * scale * vec_ref[4:5, :] + vec_ref[5:6, :]).astype(BF)
            hand_n2(i).start()
            gather.tick(clock + 2 * slabs + i)
            return carry
        lax.fori_loop(0, slabs, second_norm, 0)
        for i in range(slabs):
            hand_attn(i).wait_send()
        clock = clock + 3 * slabs

        def more(index, carry):
            gather.tick(index)
            return carry
        lax.fori_loop(clock, max(gather.ticks, clock), more, 0)

        def mask_rows(i, carry):
            cross_y.wait(i)
            g = flag_rows(flags_ref, at_slab(i, piece), 0, cols) * y_buf[i].astype(F32)
            y_buf[i] = g.astype(BF)
            hand_y(i).start()
            return carry + total_rows(g)
        zero = jnp.zeros((1, cols), F32)
        d_b_down = lax.fori_loop(0, PIECES, mask_rows, zero)
        for i in range(slabs):
            hand_n2(i).wait_recv()
        for i in range(PIECES):
            hand_y(i).wait_recv()

        assert 2 * waves == 2 * per
        d_b_up = [[], []]
        for block_j in range(spans_of):
            across = slice(block_j * span, block_j * span + span)
            for slot in range(2):
                begin = block_j == 0 and slot == 0
                last = block_j == spans_of - 1 and slot == 1
                base = clock if block_j else 0

                def mlp(index, carry, slot=slot, across=across, begin=begin, last=last, base=base,
                        block_j=block_j):
                    b = lax.rem(index + waves // 2, waves)
                    at = at_slab(b, wave)
                    n2 = second[pl.ds(b * (wave // slab), wave // slab)].reshape(wave, cols)
                    g = y_buf[pl.ds(b * (wave // piece), wave // piece)].reshape(wave, cols)
                    up, down = weight(slot, 2)[:, across], weight(slot, 3)[across]
                    pre = dg(n2, up, 1, 0) + small_buf[slot, 0:1, across]
                    cdf = 0.5 * (1.0 + lax.erf(pre * (0.5 ** 0.5)))
                    pdf = jnp.exp(-0.5 * pre * pre) * 0.3989422804014327
                    act = (pre * cdf).astype(BF)
                    grad = (dg(g, down, 1, 1) * (cdf + pre * pdf)).astype(BF)
                    hidden[at, :] = act
                    grad_pre[at, :] = grad
                    ahead, behind = dg(act, down, 1, 0), dg(grad, up, 1, 1)
                    if not begin:
                        ahead, behind = ahead + mlp_sum[at, :], behind + gn2_sum[at, :]
                    if last:
                        @pl.when(b >= waves // 2)
                        def _():
                            for k in range(wave // slab):
                                i = (b - waves // 2) * (wave // slab) + k
                                rows_k = slice(k * slab, k * slab + slab)
                                given[0, i] = behind[rows_k].astype(BF)
                                given[1, i] = ahead[rows_k].astype(BF)
                                hand_gn2(i).start()
                                hand_mlp(i).start()

                        @pl.when(b < waves // 2)
                        def _():
                            mlp_sum[at, :] = ahead
                            gn2_sum[at, :] = behind
                    else:
                        mlp_sum[at, :] = ahead
                        gn2_sum[at, :] = behind
                    if block_j:
                        reduce.tick(base + index)
                    return carry + total_rows(grad.astype(F32))
                d_b_up[slot].append(lax.fori_loop(0, waves, mlp, jnp.zeros((1, span), F32)))
                if block_j:
                    clock += waves
                at_chunk = 2 * per * block_j
                split = (4, per, rows, cols)
                out = dg(hidden[...], y_buf[...].reshape(seq, cols), 0, 0)
                reduce.g[slot, :, at_chunk:at_chunk + per] = out.astype(BF).reshape(split)
                out = dg(grad_pre[...], second[...].reshape(seq, cols), 0, 0)
                reduce.g[slot, :, at_chunk + per:at_chunk + 2 * per] = out.astype(BF).reshape(split)
            if block_j == 0:
                clock = -2
        for i in range(slabs):
            hand_mlp(i).wait_recv()
            hand_gn2(i).wait_recv()

        def result(i, carry):
            at = at_slab(i)
            value = (residual[i] + mlp_sum[at, :] + vec_ref[6:7, :] + taken[1, i].astype(F32))
            out_rows[i] = (flag_rows(flags_ref, at, 0, cols) * value).astype(BF)
            cross_out.start(i)
            reduce.tick(clock + i)
            return carry
        lax.fori_loop(0, slabs, result, 0)
        clock += slabs

        def second_back(i, carry):
            d_gain, d_bias, d_out = carry
            at = at_slab(i)
            grad = gn2_sum[at, :] + taken[0, i].astype(F32)
            center, scale = stats(residual[i])
            unit = center * scale
            turned = grad * vec_ref[4:5, :]
            inside = (turned - jnp.mean(turned, -1, keepdims=True)
                      - unit * jnp.mean(turned * unit, -1, keepdims=True))
            value = y_buf[i].astype(F32) + scale * inside
            gn2_sum[at, :] = value
            gres[i] = value.astype(BF)
            hand_res(i).start()
            reduce.tick(clock + i)
            return (d_gain + total_rows(grad * unit), d_bias + total_rows(grad),
                    d_out + total_rows(value))
        d_gain, d_bias, d_out = lax.fori_loop(0, slabs, second_back, (zero, zero, zero))
        clock += slabs
        for turn in range(2):
            sums[turn, 0] = jnp.zeros((8, cols), F32)
        for k, line in enumerate((d_out, d_gain, d_bias, d_b_down)):
            sums[0, 0, k:k + 1, :] = line
        shard_row = [4 + 2 * me.c + t_odd, 5 + 2 * me.c - t_odd]
        for slot in range(2):
            sums[0, 0, pl.ds(shard_row[slot], 1), :] = jnp.concatenate(d_b_up[slot], 1)
        hop(0, 0).start()
        for i in range(slabs):
            hand_res(i).wait_recv()
        res_all = gres[...].reshape(seq, cols)
        for slot in range(2):
            at = slice(slot * local, slot * local + local)
            do_ref[at, :] = dg(weight(slot, 1), res_all, 1, 1).astype(BF)
            out = dg(ctx_ref[at, :], res_all, 1, 0)
            reduce.g[slot, :, early - counts[1]:early] = (
                out.astype(BF).reshape(4, counts[1], rows, cols))
        for k in range(counts[1]):
            reduce.tick(jnp.int32(clock + k))
        clock += counts[1]

        def attention_back(index, carry):
            reduce.tick(clock + index)
            for k in range(hops):
                @pl.when(index == 4 * k + 3)
                def _(k=k):
                    hop_on(k, 0)
            part = lax.rem(index, narrow_parts)
            head = index // narrow_parts
            slot, at_head = head // heads, lax.rem(head, heads)

            def feature(i):
                return pl.ds(pl.multiple_of((i * heads + at_head) * HEAD_DIM, HEAD_DIM), HEAD_DIM)

            at = at_slab(part, narrow)
            at_row = pl.ds(pl.multiple_of(head * HEAD_DIM, HEAD_DIM), HEAD_DIM)
            k, v = qkv_ref[slot, feature(1), :], qkv_ref[slot, feature(2), :]
            q = qkv_ref[slot, feature(0), at] * jnp.asarray(HEAD_DIM ** (-0.5), BF)
            dob = do_ref[at_row, at]
            inner = jnp.sum(dob.astype(F32) * ctx_ref[at_row, at].astype(F32), 0, keepdims=True)
            scores = dg(jnp.concatenate([k, bias_ref[...]], 0),
                        jnp.concatenate([q, first_row(narrow)], 0), 0, 0)
            probs = jnp.exp(scores - lse_ref[head, :, at])
            ds = (probs * (dg(v, dob, 0, 0) - inner)).astype(BF)
            dv = dg(dob, probs.astype(BF), 1, 1)
            dk = dg(q, ds, 1, 1)
            qkv_ref[slot, feature(0), at] = (dg(k, ds, 1, 0) * HEAD_DIM ** (-0.5)).astype(BF)

            @pl.when(part == 0)
            def _():
                dk_ref[...] = dk
                dv_ref[...] = dv

            @pl.when(part > 0)
            def _():
                dk_ref[...] += dk
                dv_ref[...] += dv

            @pl.when(part == narrow_parts - 1)
            def _():
                qkv_ref[slot, feature(1), :] = dk_ref[...].astype(BF)
                qkv_ref[slot, feature(2), :] = dv_ref[...].astype(BF)
            return carry
        lax.fori_loop(0, bubble, attention_back, 0)
        clock += bubble

        quarter = wide // 4
        n1_all = normed[...].reshape(seq, cols)
        for slot in range(2):
            for i in range(4):
                out = dg(qkv_ref[slot, i * quarter:(i + 1) * quarter, :], n1_all, 1, 0)
                reduce.g[slot, i, early:] = out.astype(BF).reshape(counts[0], rows, cols)
        flat = jnp.ones((8, seq), BF)
        for slot in range(2):
            line = dg(flat, qkv_ref[slot], 1, 1)[0:1]
            line = jnp.concatenate([line[:, :third], line[:, 2 * third:],
                                    jnp.zeros((1, cols - 2 * third), F32)], 1)
            sums[1, 0, pl.ds(shard_row[slot], 1), :] = line

        def partial(start):
            at = pl.ds(pl.multiple_of(start, TALL), TALL)
            return (dg(qkv_ref[0, :, at], weight(0, 0), 0, 0)
                    + dg(qkv_ref[1, :, at], weight(1, 0), 0, 0))

        talls = own // TALL

        def other_back(i, carry):
            reduce.tick(clock + i)
            part = partial(own + i * TALL).astype(BF)
            for k in range(TALL // slab):
                given[1, i * (TALL // slab) + k] = part[k * slab:(k + 1) * slab]
                hand_gn1(i * (TALL // slab) + k).start()
            return carry
        for i in range(slabs):
            hand_mlp(i).wait_send()
        lax.fori_loop(0, talls, other_back, 0)
        clock += talls

        def own_back(i, carry):
            reduce.tick(clock + i)
            mlp_sum[at_slab(i, TALL), :] = partial(i * TALL)
            return carry
        lax.fori_loop(0, talls, own_back, 0)
        clock += talls

        def first_back(i, carry):
            d_mask, d_gain, d_bias = carry
            reduce.tick(clock + i)
            at = at_slab(i)
            hand_gn1(i).wait_recv()
            grad = mlp_sum[at, :] + taken[1, i].astype(F32)
            center, scale = stats(block_ref[at, :])
            unit = center * scale
            turned = grad * vec_ref[1:2, :]
            inside = (turned - jnp.mean(turned, -1, keepdims=True)
                      - unit * jnp.mean(turned * unit, -1, keepdims=True))
            grad_in = gn2_sum[at, :] + scale * inside
            valid = flag_rows(flags_ref, at, 0, cols)
            masked = flag_rows(flags_ref, at, 1, cols)
            kept = valid * (1.0 - masked) * grad_in
            mlp_sum[pl.ds(pl.multiple_of(own + i * slab, slab), slab), :] = kept
            stage[i] = kept.astype(BF)
            cross_p.start(i)
            return (d_mask + total_rows(valid * masked * grad_in),
                    d_gain + total_rows(grad * unit), d_bias + total_rows(grad))
        lines = lax.fori_loop(0, slabs, first_back, (zero, zero, zero))
        clock += slabs
        for k in range(3):
            sums[1, 0, k:k + 1, :] = lines[k]
        gp_copy = pltpu.make_async_copy(mlp_sum.at[pl.ds(own, own)], gp_out, local_sem.at[5])
        gp_copy.start()
        hop(0, 1).start()

        def step_on(index, carry):
            reduce.tick(index)
            for k in range(hops):
                @pl.when(index == clock + HOP * k + HOP - 1)
                def _(k=k):
                    hop_on(k, 1)
            return carry
        lax.fori_loop(clock, max(reduce.ticks, clock + HOP * hops), step_on, 0)
        small_out[0] = sums[0, hops]
        small_out[1] = sums[1, hops]
        for i in range(PIECES):
            cross_out.wait(i)
            cross_p.wait(i)
        out_copy = pltpu.make_async_copy(out_buf, out_out, local_sem.at[6])
        p_copy = pltpu.make_async_copy(p_buf, p_out, local_sem.at[7])
        out_copy.start()
        p_copy.start()
        for k in range(hops):
            hop(k, 0).wait_send()
            hop(k, 1).wait_send()
        for i in range(PIECES):
            hand_n1(i).wait_send()
            hand_y(i).wait_send()
        for i in range(slabs):
            for each in (hand_n2, hand_res, hand_gn2, hand_gn1):
                each(i).wait_send()
        for each in (cross_x, cross_y, cross_out, cross_p):
            each.drain()
        home(lambda: bias_pull(True).wait_send())

        def sent_bias():
            bias_pull(False).wait_send()
            bias_relay.wait_send()
        away(sent_bias)
        gather.finish()
        outs = [(early - counts[1], counts[1], fo), (early, counts[0], fq)]
        for k in range(spans_of):
            outs += [(2 * per * k, per, fd.at[k]), (2 * per * k + per, per, fu.at[k])]
        reduce.finish(outs)
        for cp in (gp_copy, out_copy, p_copy):
            cp.wait()

    dma = pltpu.SemaphoreType.DMA
    vmem = pl.BlockSpec(memory_space=pltpu.VMEM)
    shape = jax.ShapeDtypeStruct
    slab_shape = (slabs, slab, cols)
    half_shape = (own, cols)
    rows_shape = patches.shape
    return pl.pallas_call(
        kernel, in_specs=[ANY] * 6 + [vmem] * 10, out_specs=[ANY, vmem] + [ANY] * 6,
        out_shape=[shape(half_shape, F32), shape((2, 8, cols), F32),
                   shape((4, counts[1], rows, cols), BF),
                   shape((spans_of, 4, per, rows, cols), BF),
                   shape((spans_of, 4, per, rows, cols), BF),
                   shape((4, counts[0], rows, cols), BF), shape(rows_shape, BF),
                   shape(rows_shape, BF)],
        scratch_shapes=[
            pltpu.VMEM(rows_shape, BF), pltpu.VMEM((2 * PIECES,) + rows_shape[1:], BF),
            pltpu.VMEM((2,) + rows_shape, BF), pltpu.VMEM((2, 8, cols), F32),
            pltpu.VMEM((2, 4, n, rows, cols), BF), pltpu.VMEM((2 * slabs, slab, cols), BF),
            pltpu.VMEM((2, slabs, slab, cols), BF), pltpu.VMEM((2, slabs, slab, cols), BF),
            pltpu.VMEM((slabs, slab, cols), F32), pltpu.VMEM(half_shape, F32),
            pltpu.VMEM((seq, span), BF), pltpu.VMEM((seq, span), BF),
            pltpu.VMEM((seq, cols), F32), pltpu.VMEM((seq, cols), F32),
            pltpu.VMEM((2 * slabs, slab, cols), BF), pltpu.VMEM((2, wide, seq), BF),
            pltpu.VMEM((2 * local, seq), BF), pltpu.VMEM((2 * heads, 1, seq), F32),
            pltpu.VMEM((2 * local, seq), BF)] + [pltpu.VMEM(rows_shape, BF)] * 4
        + [pltpu.VMEM((HEAD_DIM, seq), F32)] * 2
        + [pltpu.VMEM((2, hops + 1, 8, cols), F32), pltpu.VMEM((2, hops, 8, cols), F32),
           pltpu.VMEM((8, cols), F32), pltpu.VMEM((8, cols), F32), pltpu.VMEM((16, seq), BF),
           dma((Gather.SEMS, n)), dma((Gather.SEMS, n)), dma((9,))]
        + Cross.sems() * 4 + [dma((14, PIECES)), dma((14, PIECES))]
        + Reduce.scratch(chunks, rows, cols),
        compiler_params=pltpu.CompilerParams(collective_id=1, **COMM), name="layer",
    )(patches, out_grad, *shards_in, flags, b_qv, b_up, *vectors)


def rest(w, total):
    if w.n_dp > 8:
        groups = [[r + 8 * g for g in range(w.n_dp // 8)] for r in range(8)]
        total = lax.psum(total, "dp", axis_index_groups=groups)
    return total


class Wires:
    def __init__(self, n_dp, n_tp):
        assert n_tp == 4 and n_dp % 8 == 0
        self.n_dp, self.n_tp = n_dp, n_tp
        self.core = [(d * n_tp + t, (d ^ 1) * n_tp + t) for d in range(n_dp) for t in range(n_tp)]

    def other(self, value):
        return lax.ppermute(value, AXES, self.core)


def shards(w, patches, validity, mask_pos, mask_token, ln1_gain, ln1_bias, w_qkv, b_qv, w_out,
           b_out, ln2_gain, ln2_bias, w_up, b_up, w_down, b_down, out_grad):
    d, t = lax.axis_index("dp"), lax.axis_index("tp")
    c = d & 1
    rows, width = patches.shape
    seq = validity.shape[1]
    local = w_qkv.shape[2]
    heads = local // HEAD_DIM
    wide = 3 * local
    swapped = ((d ^ t) & 1) == 1
    pieces = lambda v: v.reshape(PIECES, rows // PIECES, width)
    chunk = lambda v, k: v.reshape(v.shape[:-2] + (4, -1, k, width))

    bucket = t >> 1
    flags = jnp.stack([lax.dynamic_index_in_dim(validity, bucket, 0, False),
                       lax.dynamic_index_in_dim(mask_pos, bucket, 0, False)])
    flags = jnp.where(swapped, w.other(flags), flags)
    own_flags = lax.dynamic_slice_in_dim(flags, c * rows, rows, 1)
    other_flags = lax.dynamic_slice_in_dim(flags, (1 - c) * rows, rows, 1)
    valid_row = jnp.concatenate([own_flags[0], other_flags[0]]).astype(BF)
    mask_row = jnp.concatenate([own_flags[1], other_flags[1]]).astype(BF)
    flags = jnp.zeros((16, seq), BF).at[0].set(valid_row).at[1].set(mask_row)
    turned = w_qkv.transpose(1, 2, 0).reshape(wide, width)
    grad_patches, totals, f_out, f_up, f_down, f_qkv, output, moved = layer(
        pieces(patches), pieces(out_grad),
        [chunk(turned, CHUNK), chunk(w_out, CHUNK), chunk(w_up, CHUNK), chunk(w_down, CHUNK)],
        flags, b_qv, b_up, (mask_token, ln1_gain, ln1_bias, b_out, ln2_gain, ln2_bias, b_down))
    output = output.reshape(rows, width)
    grad_patches = jnp.where(swapped, moved.reshape(rows, width).astype(F32), grad_patches)
    totals = rest(w, totals)
    bias_rows = lax.dynamic_index_in_dim(totals, 4 + t, 1, False)
    whole = lambda v: rest(w, v.reshape(-1, width).astype(F32))
    grad_w_qkv = whole(f_qkv).reshape(3, local, width).transpose(2, 0, 1)
    return (output, grad_patches, totals[1, 0], totals[1, 1], totals[1, 2], grad_w_qkv,
            bias_rows[1, :2 * local].reshape(2, local), whole(f_out), totals[0, 0], totals[0, 1],
            totals[0, 2], whole(f_up).T, bias_rows[0], whole(f_down), totals[0, 3])


def solution(mesh):
    w = Wires(mesh.shape["dp"], mesh.shape["tp"])
    rows, cols = P(AXES, None), P(None, "tp")
    return jax.shard_map(
        lambda *args: shards(w, *args),
        mesh=mesh,
        in_specs=(rows, P("dp", None), P("dp", None), P(), P(), P(), P(None, None, "tp"), cols,
                  P("tp", None), P(), P(), P(), cols, P("tp"), P("tp", None), P(), rows),
        out_specs=(rows, rows, P(), P(), P(), P(None, None, "tp"), cols, P("tp", None), P(), P(),
                   P(), cols, P("tp"), P("tp", None), P()),
        check_vma=False,
    )
```
